32 devices in a mesh: parts: 2 (over y), tile: 8 (over z, x), cond: 2 (over core).
Axes of the slice: x: 2, y: 2, z: 4, core: 2. Of those that a mesh axis runs over, the one named last changes fastest.
Arguments:
- mask: bfloat16 [16, 256, 256], P(('parts', 'tile')), parts along dimension 0, may hold values from -1 to 1
- kernels: bfloat16 [8, 24, 64, 128], P('cond'), may hold values from -6 to 6
- socs_weight: float32 [8, 24], P('cond'), may hold values from 0.02 to 1
- dose: float32 [8], P('cond'), may hold values from 0.8 to 1.25
- threshold: float32 [8], P('cond'), may hold values from 0.5 to 0.85
Outputs:
- band_max: float32 [16, 256, 256], P(('parts', 'tile'), 'cond'), parts along dimension 0
- band_min: float32 [16, 256, 256], P(('parts', 'tile'), 'cond'), parts along dimension 0
The draws below stay inside these ranges and needn't reach their ends.
There are 2 independent parts, one for each index of `parts`. The reference program is written for one: setup_inputs(seed, part) draws one part's arguments, and reference() takes and returns one part's arrays. A program takes and returns all parts, laid end to end along the dimension named above; an argument that names none is the same for every part. Nothing has to cross between parts.
All inputs are finite; a program needn't handle non-finite values.
Results may differ from the reference program's by a relative error of at most 0.0068.
Values may be sent and summed in bfloat16 or wider, within the bound.
A program may use at most 64 MiB of HBM per device.

```python
import math
import jax
import jax.numpy as jnp
from jax import lax

CORE = 256
MARGIN = 64
BLUR = 8
BAND = 64
KERN = 24
COND = 8
TILES = 8
N_TILE = 8


def levels(own_key, shape, split, smallest, largest):
    def one(dim, shards_of):
        heights = jax.random.uniform(jax.random.fold_in(jax.random.fold_in(own_key, 6), dim), (shards_of,), jnp.float32, smallest / len(split), largest / len(split))
        return jnp.repeat(jnp.exp(heights), shape[dim] // shards_of).reshape((-1,) + (1,) * (len(shape) - dim - 1))

    factor_of = one(*split[0])
    for cut in split[1:]:
        factor_of = factor_of * one(*cut)
    return factor_of


def normal_values(stream_key, shape, scale, bound, cuts=(), held_as=jnp.bfloat16):
    loudness = levels(stream_key, shape, cuts, -0.22, 0.18) if cuts else 1.0
    array = jax.random.normal(stream_key, shape, jnp.float32) * scale * loudness
    return jnp.minimum(jnp.maximum(array, -bound), bound).astype(held_as)


def setup_inputs(seed: int = 0, part: int = 0) -> dict:
    key_of = jax.random.split(jax.random.key(seed), 6)
    own_keys = jax.random.split(jax.random.fold_in(key_of[5], part), 6)
    mask = jnp.clip(jax.random.uniform(own_keys[0], (TILES, CORE, CORE), jnp.float32, -1.0, 1.0) * levels(own_keys[0], (TILES, CORE, CORE), ((0, 8),), -0.4, 0.0), -1.0, 1.0).astype(jnp.bfloat16)
    kernels = normal_values(key_of[1], (COND, KERN, BAND, 2 * BAND), 1.0, 6.0, ((0, 2),))
    socs_weight = jnp.clip(jnp.exp(math.log(1.0) - 3.912023 * jax.random.uniform(key_of[2], (COND, KERN), jnp.float32) ** levels(key_of[2], (COND, KERN), ((0, 2),), -0.2, 0.2)), 0.02, 1.0)
    dose = jnp.clip(0.8 + 0.45 * jax.random.uniform(key_of[3], (COND,), jnp.float32) ** levels(key_of[3], (COND,), ((0, 2),), -0.2, 0.2), 0.8, 1.25)
    threshold = jnp.clip(0.5 + 0.35000002 * jax.random.uniform(key_of[4], (COND,), jnp.float32) ** levels(key_of[4], (COND,), ((0, 2),), -0.2, 0.2), 0.5, 0.85)
    return dict(mask=mask, kernels=kernels, socs_weight=socs_weight, dose=dose, threshold=threshold)


diffusion = 2.0
steepness = 8.0


def phase_table(first, count, pad_width, band_width):
    pixel_index = jnp.arange(count, dtype=jnp.int32) + first
    freq_index = (jnp.arange(band_width, dtype=jnp.int32) - band_width // 2) % pad_width
    turn_count = (pixel_index[:, None] * freq_index[None, :]) % pad_width
    angle_grid = turn_count.astype(jnp.float32) * (2.0 * math.pi / pad_width)
    return jnp.cos(angle_grid).astype(jnp.bfloat16), jnp.sin(angle_grid).astype(jnp.bfloat16)


def blur_table(core):
    offset_grid = jnp.arange(core + 2 * BLUR, dtype=jnp.int32)[None, :] - jnp.arange(core, dtype=jnp.int32)[:, None] - BLUR
    distance = offset_grid.astype(jnp.float32)
    taps_grid = jnp.exp(-distance * distance / (2.0 * diffusion * diffusion))
    taps_grid = jnp.where(jnp.abs(offset_grid) <= BLUR, taps_grid, jnp.zeros_like(taps_grid))
    reach_grid = jnp.arange(-BLUR, BLUR + 1, dtype=jnp.int32).astype(jnp.float32)
    total_taps = jnp.sum(jnp.exp(-reach_grid * reach_grid / (2.0 * diffusion * diffusion)))
    return taps_grid / total_taps


def make_tables(core, band_width):
    pad_width = core + 2 * MARGIN
    cos_in, sin_in = phase_table(0, pad_width, pad_width, band_width)
    cos_out, sin_out = phase_table(MARGIN - BLUR, core + 2 * BLUR, pad_width, band_width)
    return cos_in, sin_in, cos_out, sin_out, blur_table(core)


def expose(window, kernel_set, weights, dose_one, threshold_one, tables):
    cos_in, sin_in, cos_out, sin_out, blur_rows = tables
    pad_width = window.shape[0]
    band_width = cos_in.shape[1]
    hp = lax.Precision.HIGHEST
    part_real = jnp.dot(cos_in.T, window, preferred_element_type=jnp.float32).astype(jnp.bfloat16)
    part_imag = (-jnp.dot(sin_in.T, window, preferred_element_type=jnp.float32)).astype(jnp.bfloat16)
    spec_real = (jnp.dot(part_real, cos_in, preferred_element_type=jnp.float32) + jnp.dot(part_imag, sin_in, preferred_element_type=jnp.float32)) / pad_width
    spec_imag = (jnp.dot(part_imag, cos_in, preferred_element_type=jnp.float32) - jnp.dot(part_real, sin_in, preferred_element_type=jnp.float32)) / pad_width
    group_size = min(8, kernel_set.shape[0])
    kernel_groups = kernel_set.reshape(-1, group_size, band_width, 2 * band_width)
    weight_groups = weights.reshape(-1, group_size)
    cos_wide = cos_out.astype(jnp.float32)
    sin_wide = sin_out.astype(jnp.float32)

    def group_power(packed):
        kernel_part, weight_part = packed
        kern_real = kernel_part[:, :, :band_width].astype(jnp.float32)
        kern_imag = kernel_part[:, :, band_width:].astype(jnp.float32)
        prod_real = (spec_real * kern_real - spec_imag * kern_imag).astype(jnp.bfloat16).astype(jnp.float32)
        prod_imag = (spec_real * kern_imag + spec_imag * kern_real).astype(jnp.bfloat16).astype(jnp.float32)
        half_real = (jnp.einsum('nfg,yg->nfy', prod_real, cos_wide, precision=hp) - jnp.einsum('nfg,yg->nfy', prod_imag, sin_wide, precision=hp)).astype(jnp.bfloat16).astype(jnp.float32)
        half_imag = (jnp.einsum('nfg,yg->nfy', prod_real, sin_wide, precision=hp) + jnp.einsum('nfg,yg->nfy', prod_imag, cos_wide, precision=hp)).astype(jnp.bfloat16).astype(jnp.float32)
        field_real = (jnp.einsum('xf,nfy->nxy', cos_wide, half_real, precision=hp) - jnp.einsum('xf,nfy->nxy', sin_wide, half_imag, precision=hp)) / band_width
        field_imag = (jnp.einsum('xf,nfy->nxy', cos_wide, half_imag, precision=hp) + jnp.einsum('xf,nfy->nxy', sin_wide, half_real, precision=hp)) / band_width
        power = field_real * field_real + field_imag * field_imag
        return jnp.tensordot(weight_part, power, axes=1, precision=hp)

    intensity = jnp.sum(lax.map(group_power, (kernel_groups, weight_groups)), axis=0) / jnp.sum(weights)
    blurred = jnp.dot(jnp.dot(blur_rows, intensity, precision=hp), blur_rows.T, precision=hp)
    return jax.nn.sigmoid(steepness * (dose_one * blurred - threshold_one))


def reference(mask, kernels, socs_weight, dose, threshold):
    count = mask.shape[0]
    core = mask.shape[1]
    columns = min(8, N_TILE // 2)
    grid_rows = count // columns
    rotate = columns // 2
    holder = (jnp.arange(count, dtype=jnp.int32) - rotate) % count
    placed = mask[holder]
    region_plane = placed.reshape(grid_rows, columns, core, core).transpose(0, 2, 1, 3).reshape(grid_rows * core, columns * core)
    padded = jnp.pad(region_plane, MARGIN)
    tables = make_tables(core, kernels.shape[2])
    pad_width = core + 2 * MARGIN

    def one_tile(index):
        position = (index + rotate) % count
        top_row = ((position // columns) * core).astype(jnp.int32)
        left_col = ((position % columns) * core).astype(jnp.int32)
        window = lax.dynamic_slice(padded, (top_row, left_col), (pad_width, pad_width))

        def one_condition(packed):
            kernel_set, weights, dose_one, threshold_one = packed
            return expose(window, kernel_set, weights, dose_one, threshold_one, tables)

        resist = lax.map(one_condition, (kernels, socs_weight, dose, threshold))
        return jnp.max(resist, axis=0), jnp.min(resist, axis=0)

    highest, lowest = lax.map(one_tile, jnp.arange(count, dtype=jnp.int32))
    return highest, lowest
```

```python
import jax
import jax.numpy as jnp
import ml_dtypes
import numpy as np
from jax import lax
from jax.experimental import pallas as pl
from jax.experimental.pallas import tpu as pltpu
from jax.sharding import PartitionSpec as P

MARGIN = 64
BLUR = 8
GROUP = 4
AHEAD = 2

diffusion = 2.0
steepness = 8.0
bf16 = jnp.bfloat16
f32 = jnp.float32


def trig(turns, period):
    angle = 2.0 * np.pi * (turns % period) / period
    return np.cos(angle), np.sin(angle)


def split(table):
    high = table.astype(ml_dtypes.bfloat16)
    low = (table - high.astype(np.float64)).astype(ml_dtypes.bfloat16)
    return high, low


def make_tables(core, band):
    pad = core + 2 * MARGIN
    grid = 2 * band
    freq = np.arange(band) - band // 2
    cos_in, sin_in = trig(np.arange(pad)[:, None] * freq[None, :], pad)
    order = np.r_[MARGIN : MARGIN + core, 0:MARGIN, MARGIN + core : pad]
    row_table = np.concatenate([cos_in[order].T, -sin_in[order].T], axis=0)
    both = np.concatenate([cos_in, sin_in], axis=1)
    left, inner, right = both[:MARGIN], both[MARGIN : MARGIN + core], both[MARGIN + core :]
    blank = np.zeros((core - MARGIN, 2 * band))
    send_table = np.concatenate(
        [inner, np.concatenate([blank, left]), np.concatenate([right, blank])], axis=1
    )
    zero = np.zeros_like(left)
    side_table = np.block([[left, zero], [zero, left], [right, zero], [zero, right]])
    cos_grid, sin_grid = trig(np.arange(grid)[:, None] * freq[None, :], grid)
    half_table = np.block([[cos_grid.T, sin_grid.T], [-sin_grid.T, cos_grid.T]])
    field_table = np.block([[cos_grid, -sin_grid], [sin_grid, cos_grid]])
    pixel = np.arange(core + 2 * BLUR) + MARGIN - BLUR
    phase = pixel[:, None] / pad - np.arange(grid)[None, :] / grid
    waves = np.arange(1, band)
    interp = (1.0 + 2.0 * np.cos(2.0 * np.pi * phase[:, :, None] * waves).sum(-1)) / grid
    offset = np.arange(core + 2 * BLUR)[None, :] - np.arange(core)[:, None] - BLUR
    taps = np.exp(-(offset**2) / (2.0 * diffusion**2)) * (np.abs(offset) <= BLUR)
    reach = np.arange(-BLUR, BLUR + 1)
    taps = taps / np.exp(-(reach**2) / (2.0 * diffusion**2)).sum()
    rise = taps @ interp
    high, low = split(rise)
    rise_rows = np.concatenate([high, high, low], axis=1)
    rise_cols = np.concatenate([high.T, high.T, low.T], axis=0)
    tables = (row_table, send_table, side_table, half_table, field_table)
    return (*(t.astype(ml_dtypes.bfloat16) for t in tables), rise_rows, rise_cols)


def neighbours():
    count = lax.axis_size("tile")
    columns = min(8, count // 2)
    rows = count // columns
    me = lax.axis_index("tile")
    position = lax.rem(me + columns // 2, count)
    column = lax.rem(position, columns)
    row = lax.div(position, columns)
    found = []
    for down in (-1, 0, 1):
        for right in (-1, 0, 1):
            if down == 0 and right == 0:
                continue
            flag = (row + down >= 0) & (row + down < rows)
            flag = flag & (column + right >= 0) & (column + right < columns)
            there = lax.rem(me + down * columns + right + count, count)
            found.append((down, right, flag, there))
    return found


def slot(down, right):
    return (0 if down < 0 else 1, right % 3) if down else (0 if right < 0 else 1,)


def high_low(value):
    high = value.astype(bf16)
    return high, (value - high.astype(f32)).astype(bf16)


def dot(a, b):
    return jnp.dot(a, b, preferred_element_type=f32)


def body(
    mask_hbm,
    kern_hbm,
    weight_hbm,
    dose_hbm,
    threshold_hbm,
    row_hbm,
    send_hbm,
    side_hbm,
    half_hbm,
    field_hbm,
    rise_rows_hbm,
    rise_cols_hbm,
    high_out,
    low_out,
    weight,
    dose,
    threshold,
    tile,
    kern,
    row_table,
    send_table,
    side_table,
    half_table,
    field_table,
    rise_rows,
    rise_cols,
    rows_out,
    rows_in,
    side_out,
    side_in,
    level,
    arrived,
    load_sem,
    halo_send,
    halo_recv,
    swap_send,
    swap_recv,
    plain,
    turned,
):
    core = mask_hbm.shape[1]
    conds, kerns, band, _ = kern_hbm.shape
    grid = 2 * band
    n_cond = lax.axis_size("cond")
    me = lax.axis_index("cond")
    around = neighbours()

    loads = [
        pltpu.make_async_copy(src, dst, load_sem.at[i])
        for i, (src, dst) in enumerate(
            (
                (mask_hbm.at[0], tile),
                (row_hbm, row_table),
                (send_hbm, send_table),
                (kern_hbm, kern),
                (weight_hbm, weight),
                (dose_hbm, dose),
                (threshold_hbm, threshold),
                (side_hbm, side_table),
                (half_hbm, half_table),
                (field_hbm, field_table),
                (rise_rows_hbm, rise_rows),
                (rise_cols_hbm, rise_cols),
            )
        )
    ]
    for load in loads[:3]:
        load.start()

    barrier = pltpu.get_barrier_semaphore()
    for _, _, flag, there in around:

        @pl.when(flag)
        def _():
            pl.semaphore_signal(barrier, inc=1, device_id={"tile": there})

    for step in range(1, n_cond):
        pl.semaphore_signal(barrier, inc=1, device_id={"cond": lax.rem(me + step, n_cond)})
    for load in loads[3:]:
        load.start()
    for down, right, flag, _ in around:

        @pl.when(jnp.logical_not(flag))
        def _():
            buffer = rows_in if down else side_in
            at = slot(down, right)
            buffer[at] = jnp.zeros(buffer.shape[len(at) :], bf16)

    for load in loads[:3]:
        load.wait()
    middle = dot(row_table[:, :core], tile[...]).astype(bf16)
    for at, first in ((0, 0), (1, core - MARGIN)):
        block = dot(tile[first : first + MARGIN, :], send_table[...]).astype(bf16)
        for lanes in range(3):
            rows_out[at, lanes] = block[:, lanes * 2 * band : (lanes + 1) * 2 * band]
        strip = middle[:, first : first + MARGIN]
        side_out[at] = jnp.concatenate([strip[:band], strip[band:]], axis=1)
    peers = n_cond - 1
    for _, _, flag, _ in around:
        peers = peers + flag.astype(jnp.int32)
    pl.semaphore_wait(barrier, peers)

    def halo(i):
        down, right, flag, there = around[i]
        outgoing, incoming = (rows_out, rows_in) if down else (side_out, side_in)
        return pltpu.make_async_remote_copy(
            src_ref=outgoing.at[slot(down, right)],
            dst_ref=incoming.at[slot(-down, -right)],
            send_sem=halo_send.at[i],
            recv_sem=halo_recv.at[len(around) - 1 - i],
            device_id={"tile": there},
        )

    def arrival(i):
        down, right, flag, there = around[i]
        outgoing, incoming = (rows_out, rows_in) if down else (side_out, side_in)
        return pltpu.make_async_remote_copy(
            src_ref=outgoing.at[slot(down, right)],
            dst_ref=incoming.at[slot(down, right)],
            send_sem=halo_send.at[i],
            recv_sem=halo_recv.at[i],
            device_id={"tile": there},
        )

    for i in range(len(around)):

        @pl.when(around[i][2])
        def _():
            halo(i).start()

    for load in loads[3:]:
        load.wait()
    inner = dot(middle, send_table[:, : 2 * band])
    tops = []
    for c in range(conds):
        weight_sum = weight[c, 0]
        for k in range(1, kerns):
            weight_sum = weight_sum + weight[c, k]
        gain = jnp.full((8, grid), steepness * dose[c], f32) / jnp.full((8, grid), weight_sum, f32)
        tops.append(steepness * threshold[c])
        for k in range(kerns):
            root = jnp.sqrt(gain * weight[c, k])
            scaled = kern[c, k].astype(f32) * root[0:1]
            plain[c, k] = scaled
            turned[c, k] = pltpu.roll(scaled, band, 1)

    for i in range(len(around)):

        @pl.when(around[i][2])
        def _():
            arrival(i).wait_recv()

    outer = rows_in[...].astype(f32)
    outer = (outer[:, 0] + outer[:, 1] + outer[:, 2]).reshape(2 * MARGIN, 2 * band).astype(bf16)
    sides = dot(jnp.concatenate([side_in[0], side_in[1]], axis=1), side_table[...])
    sides = jnp.concatenate([sides[:, : 2 * band], sides[:, 2 * band :]], axis=0)
    quarters = inner + dot(row_table[:, core:], outer) + sides
    quarters = quarters * (1.0 / ((core + 2 * MARGIN) * band))
    turned_quarters = pltpu.roll(quarters, band, 1)
    lane = lax.broadcasted_iota(jnp.int32, (band, 2 * band), 1)
    first = lane < band
    top, bottom = quarters[:band], quarters[band:]
    top_turned, bottom_turned = turned_quarters[:band], turned_quarters[band:]
    spec_same = jnp.where(first, top + bottom_turned, top_turned + bottom)
    spec_cross = jnp.where(first, top_turned - bottom, bottom_turned - top)

    def swap(c, step):
        return pltpu.make_async_remote_copy(
            src_ref=level.at[c],
            dst_ref=arrived.at[step - 1, c],
            send_sem=swap_send.at[step - 1, c],
            recv_sem=swap_recv.at[step - 1, c],
            device_id={"cond": lax.rem(me + step, n_cond)},
        )

    def halves(c, start, size):
        prod = [
            (spec_same * plain[c, k] + spec_cross * turned[c, k]).astype(bf16)
            for k in range(start, start + size)
        ]
        half = dot(jnp.concatenate(prod, axis=0), half_table[...]).astype(bf16)
        return [half[j * band : (j + 1) * band] for j in range(size)]

    def powers(total, pair):
        stacked = jnp.concatenate(
            [
                jnp.concatenate([h[:, :grid] for h in pair], axis=1),
                jnp.concatenate([h[:, grid:] for h in pair], axis=1),
            ],
            axis=0,
        )
        field = dot(field_table[...], stacked)
        power = field[:grid] * field[:grid] + field[grid:] * field[grid:]
        for j in range(len(pair)):
            total = total + power[:, j * grid : (j + 1) * grid]
        return total

    groups = [
        (c, start, min(GROUP, kerns - start)) for c in range(conds) for start in range(0, kerns, GROUP)
    ]
    ready = [halves(*groups[i]) for i in range(min(AHEAD, len(groups)))]
    total = None
    for i, (c, start, size) in enumerate(groups):
        if i + AHEAD < len(groups):
            ready.append(halves(*groups[i + AHEAD]))
        if start == 0:
            total = jnp.full((grid, grid), -tops[c], f32)
        half = ready[i]
        for j in range(0, size, 2):
            total = powers(total, half[j : j + 2])
        if start + size == kerns:
            level[c] = total
            for step in range(1, n_cond):
                swap(c, step).start()

    share = high_out.shape[1]
    row_part = rise_rows[pl.ds(pl.multiple_of(me * share, share), share), :]

    def include(bounds, values):
        high, low = high_low(jnp.concatenate(values, axis=0))
        wide = dot(jnp.concatenate([high, low, high], axis=1), rise_cols[...])
        high, low = high_low(wide)
        high = jnp.concatenate([high[j * grid : (j + 1) * grid] for j in range(len(values))], axis=1)
        low = jnp.concatenate([low[j * grid : (j + 1) * grid] for j in range(len(values))], axis=1)
        blurred = dot(row_part, jnp.concatenate([high, low, high], axis=0))
        for j in range(len(values)):
            one = blurred[:, j * core : (j + 1) * core]
            bounds = (one, one) if bounds is None else (
                jnp.maximum(bounds[0], one),
                jnp.minimum(bounds[1], one),
            )
        return bounds

    bounds = include(None, [level[c] for c in range(conds)])
    pieces = [(step, c) for step in range(1, n_cond) for c in range(conds)]
    for some in (pieces[:-1], pieces[-1:]):
        if some:
            for step, c in some:
                swap(c, step).wait_recv()
            bounds = include(bounds, [arrived[step - 1, c] for step, c in some])
    high_out[0] = bounds[0]
    low_out[0] = bounds[1]
    for step in range(1, n_cond):
        for c in range(conds):
            swap(c, step).wait_send()
    for i in range(len(around)):

        @pl.when(around[i][2])
        def _():
            halo(i).wait_send()


def on_device(mask, kernels, socs_weight, dose, threshold):
    core = mask.shape[1]
    conds, kerns, band, _ = kernels.shape
    n_cond = lax.axis_size("cond")
    tables = [jnp.asarray(t) for t in make_tables(core, band)]
    share = core // n_cond
    anywhere = pl.BlockSpec(memory_space=pl.ANY)
    vmem = pl.BlockSpec(memory_space=pltpu.VMEM)
    grid = 2 * band
    out = pltpu.VMEM((1, share, core), f32)
    high, low = pl.pallas_call(
        body,
        out_shape=(out, out),
        in_specs=[anywhere] * (5 + len(tables)),
        out_specs=(vmem, vmem),
        scratch_shapes=[
            pltpu.SMEM(socs_weight.shape, f32),
            pltpu.SMEM(dose.shape, f32),
            pltpu.SMEM(threshold.shape, f32),
            pltpu.VMEM((core, core), bf16),
            pltpu.VMEM(kernels.shape, bf16),
            *[pltpu.VMEM(t.shape, bf16) for t in tables],
            pltpu.VMEM((2, 3, MARGIN, 2 * band), bf16),
            pltpu.VMEM((2, 3, MARGIN, 2 * band), bf16),
            pltpu.VMEM((2, band, 2 * MARGIN), bf16),
            pltpu.VMEM((2, band, 2 * MARGIN), bf16),
            pltpu.VMEM((conds, grid, grid), f32),
            pltpu.VMEM((n_cond - 1, conds, grid, grid), f32),
            pltpu.SemaphoreType.DMA((5 + len(tables),)),
            pltpu.SemaphoreType.DMA((8,)),
            pltpu.SemaphoreType.DMA((8,)),
            pltpu.SemaphoreType.DMA((n_cond - 1, conds)),
            pltpu.SemaphoreType.DMA((n_cond - 1, conds)),
            pltpu.VMEM(kernels.shape, f32),
            pltpu.VMEM(kernels.shape, f32),
        ],
        compiler_params=pltpu.CompilerParams(collective_id=0, has_side_effects=True),
    )(mask, kernels, socs_weight, dose, threshold, *tables)
    return jax.nn.sigmoid(high), jax.nn.sigmoid(low)


def solution(mesh):
    return jax.shard_map(
        on_device,
        mesh=mesh,
        in_specs=(
            P(("parts", "tile"), None, None),
            P("cond", None, None, None),
            P("cond", None),
            P("cond"),
            P("cond"),
        ),
        out_specs=(P(("parts", "tile"), "cond", None), P(("parts", "tile"), "cond", None)),
        check_vma=False,
    )
```

```python
import functools

import jax
import jax.numpy as jnp
import ml_dtypes
import numpy as np
from jax import lax
from jax.experimental import pallas as pl
from jax.experimental.pallas import tpu as pltpu
from jax.sharding import PartitionSpec as P

MARGIN = 64
BLUR = 8
GROUP = 4
AHEAD = 2
DELAY = 2

diffusion = 2.0
steepness = 8.0
bf16 = jnp.bfloat16
f32 = jnp.float32


def trig(turns, period):
    angle = 2.0 * np.pi * (turns % period) / period
    return np.cos(angle), np.sin(angle)


def split(table):
    high = table.astype(ml_dtypes.bfloat16)
    low = (table - high.astype(np.float64)).astype(ml_dtypes.bfloat16)
    return high, low


def make_tables(core, band):
    pad = core + 2 * MARGIN
    grid = 2 * band
    freq = np.arange(band) - band // 2
    cos_in, sin_in = trig(np.arange(pad)[:, None] * freq[None, :], pad)
    order = np.r_[MARGIN : MARGIN + core, 0:MARGIN, MARGIN + core : pad]
    row_table = np.concatenate([cos_in[order].T, -sin_in[order].T], axis=0)
    both = np.concatenate([cos_in, sin_in], axis=1)
    left, inner, right = both[:MARGIN], both[MARGIN : MARGIN + core], both[MARGIN + core :]
    zero = np.zeros_like(left)
    gap = np.zeros((core - 2 * MARGIN, 2 * band))
    edges = np.concatenate([right, gap, left], axis=0)
    first_table = np.concatenate(
        [row_table[:, :core], np.concatenate([inner, edges], axis=1)], axis=0
    )
    side_table = np.block([[left, zero], [zero, left], [right, zero], [zero, right]])
    cos_grid, sin_grid = trig(np.arange(grid)[:, None] * freq[None, :], grid)
    half_table = np.block([[cos_grid.T, sin_grid.T], [-sin_grid.T, cos_grid.T]])
    field_table = np.concatenate(
        [np.concatenate([cos_grid, -sin_grid], axis=1), np.concatenate([sin_grid, cos_grid], axis=1)], axis=1
    )
    pixel = np.arange(core + 2 * BLUR) + MARGIN - BLUR
    phase = pixel[:, None] / pad - np.arange(grid)[None, :] / grid
    waves = np.arange(1, band)
    interp = (1.0 + 2.0 * np.cos(2.0 * np.pi * phase[:, :, None] * waves).sum(-1)) / grid
    offset = np.arange(core + 2 * BLUR)[None, :] - np.arange(core)[:, None] - BLUR
    taps = np.exp(-(offset**2) / (2.0 * diffusion**2)) * (np.abs(offset) <= BLUR)
    reach = np.arange(-BLUR, BLUR + 1)
    taps = taps / np.exp(-(reach**2) / (2.0 * diffusion**2)).sum()
    rise = taps @ interp
    high, low = split(rise)
    rise_rows = np.concatenate([high, low], axis=1)
    rise_cols = np.concatenate([high.T, low.T], axis=0)
    outer_rows = np.concatenate([row_table[:, core:], np.zeros((2 * band, 2 * band))], axis=1)
    later = (side_table, half_table, field_table, outer_rows, rise_cols, rise_rows)
    bounds = np.cumsum([0] + [len(t) for t in later])
    later = np.concatenate([t.astype(ml_dtypes.bfloat16) for t in later], axis=0)
    return first_table.astype(ml_dtypes.bfloat16), later, [int(n) for n in bounds]


def neighbours():
    count = lax.axis_size("tile")
    columns = min(8, count // 2)
    rows = count // columns
    me = lax.axis_index("tile")
    position = lax.rem(me + columns // 2, count)
    column = lax.rem(position, columns)
    row = lax.div(position, columns)
    found = []
    for down in (-1, 0, 1):
        for right in (-1, 0, 1):
            if down == 0 and right == 0:
                continue
            flag = (row + down >= 0) & (row + down < rows)
            flag = flag & (column + right >= 0) & (column + right < columns)
            there = lax.rem(me + down * columns + right + count, count)
            found.append((down, right, flag, there))
    return found


def slot(down, right):
    return (0 if down < 0 else 1, right % 3) if down else (0 if right < 0 else 1,)


def high_low(value):
    high = value.astype(bf16)
    return high, (value - high.astype(f32)).astype(bf16)


def dot(a, b):
    return jnp.dot(a, b, preferred_element_type=f32)


def body(
    parts,
    mask_hbm,
    kern_hbm,
    weight_hbm,
    dose_hbm,
    threshold_hbm,
    first_hbm,
    later_hbm,
    high_out,
    low_out,
    weight,
    dose,
    threshold,
    tile,
    kern,
    first_table,
    later_table,
    rows_out,
    rows_in,
    side_out,
    side_in,
    level,
    arrived,
    load_sem,
    halo_send,
    halo_recv,
    swap_send,
    swap_recv,
    plain,
    turned,
):
    core = mask_hbm.shape[1]
    conds, kerns, band, _ = kern_hbm.shape
    grid = 2 * band
    middle_of = core // 2
    n_cond = lax.axis_size("cond")
    me = lax.axis_index("cond")
    near = n_cond - 1
    sender = me == near
    around = neighbours()
    side_table, half_table, field_table, outer_rows, rise_cols, rise_rows = (
        later_table.at[pl.ds(lo, hi - lo)] for lo, hi in zip(parts[:-1], parts[1:])
    )
    row_table = first_table.at[pl.ds(0, grid)]
    inner_table = first_table.at[pl.ds(grid, core), pl.ds(0, grid)]
    edge_table = first_table.at[pl.ds(grid, core), pl.ds(grid, grid)]

    loads = [
        pltpu.make_async_copy(src, dst, load_sem.at[i])
        for i, (src, dst) in enumerate(
            (
                (mask_hbm.at[0], tile),
                (first_hbm, first_table),
                (kern_hbm, kern),
                (weight_hbm, weight),
                (dose_hbm, dose),
                (threshold_hbm, threshold),
                (later_hbm, later_table),
            )
        )
    ]
    for load in loads[:2]:
        load.start()

    barrier = pltpu.get_barrier_semaphore()
    for _, _, flag, there in around:

        @pl.when(flag)
        def _():
            pl.semaphore_signal(barrier, inc=1, device_id={"tile": there, "cond": near})

    for step in range(1, n_cond):
        pl.semaphore_signal(barrier, inc=1, device_id={"cond": lax.rem(me + step, n_cond)})
    for down, right, flag, _ in around:

        @pl.when(jnp.logical_not(flag))
        def _():
            buffer = rows_in if down else side_in
            at = slot(down, right)
            buffer[at] = jnp.zeros(buffer.shape[len(at) :], bf16)

    for load in loads[:2]:
        load.wait()
    for load in loads[2:]:
        load.start()
    strips = jnp.concatenate([tile[:MARGIN, :], tile[core - MARGIN :, :]], axis=0)
    middle = dot(row_table[...], tile[...]).astype(bf16)
    blocks = [
        dot(strips, inner_table[...]).astype(bf16),
        dot(strips[:, middle_of:], edge_table[middle_of:, :]).astype(bf16),
        dot(strips[:, :middle_of], edge_table[:middle_of, :]).astype(bf16),
    ]
    for at, first in ((0, 0), (1, core - MARGIN)):
        for lanes in range(3):
            rows_out[at, lanes] = blocks[lanes][at * MARGIN : (at + 1) * MARGIN]
        strip = middle[:, first : first + MARGIN]
        side_out[at] = jnp.concatenate([strip[:band], strip[band:]], axis=1)
    peers = n_cond - 1
    for _, _, flag, _ in around:
        peers = peers + jnp.where(flag & sender, n_cond, 0)
    pl.semaphore_wait(barrier, peers)

    def halo(i, q):
        down, right, flag, there = around[i]
        outgoing, incoming = (rows_out, rows_in) if down else (side_out, side_in)
        return pltpu.make_async_remote_copy(
            src_ref=outgoing.at[slot(down, right)],
            dst_ref=incoming.at[slot(-down, -right)],
            send_sem=halo_send.at[q, i],
            recv_sem=halo_recv.at[len(around) - 1 - i],
            device_id={"tile": there, "cond": q},
        )

    for q in range(n_cond):
        for i in range(len(around)):

            @pl.when(around[i][2] & sender)
            def _():
                halo(i, q).start()

    for load in loads[2:]:
        load.wait()
    inner = dot(middle, inner_table[...])
    tops = []
    for c in range(conds):
        weight_sum = weight[c, 0]
        for k in range(1, kerns):
            weight_sum = weight_sum + weight[c, k]
        gain = jnp.full((8, grid), steepness * dose[c], f32) / jnp.full((8, grid), weight_sum, f32)
        tops.append(steepness * threshold[c])
        for k in range(kerns):
            root = jnp.sqrt(gain * weight[c, k])
            scaled = kern[c, k].astype(f32) * root[0:1]
            plain[c, k] = scaled
            turned[c, k] = pltpu.roll(scaled, band, 1)

    for i in range(len(around)):

        @pl.when(around[i][2])
        def _():
            halo(len(around) - 1 - i, 0).wait_recv()

    outer = rows_in[...].astype(f32)
    outer = (outer[:, 0] + outer[:, 1] + outer[:, 2]).reshape(2 * MARGIN, 2 * band).astype(bf16)
    sides = dot(jnp.concatenate([side_in[0], side_in[1]], axis=1), side_table[...])
    sides = jnp.concatenate([sides[:, : 2 * band], sides[:, 2 * band :]], axis=0)
    quarters = inner + dot(outer_rows[:, : 2 * MARGIN], outer) + sides
    quarters = quarters * (1.0 / ((core + 2 * MARGIN) * band))
    turned_quarters = pltpu.roll(quarters, band, 1)
    lane = lax.broadcasted_iota(jnp.int32, (band, 2 * band), 1)
    first = lane < band
    top, bottom = quarters[:band], quarters[band:]
    top_turned, bottom_turned = turned_quarters[:band], turned_quarters[band:]
    spec_same = jnp.where(first, top + bottom_turned, top_turned + bottom)
    spec_cross = jnp.where(first, top_turned - bottom, bottom_turned - top)

    bunches = [list(range(max(conds - 2, 0)))] + [[c] for c in range(max(conds - 2, 0), conds)]
    bunches = [bunch for bunch in bunches if bunch]

    def swap(i, step):
        chosen = pl.ds(bunches[i][0], len(bunches[i]))
        return pltpu.make_async_remote_copy(
            src_ref=level.at[chosen],
            dst_ref=arrived.at[step - 1, chosen],
            send_sem=swap_send.at[step - 1, i],
            recv_sem=swap_recv.at[step - 1, i],
            device_id={"cond": lax.rem(me + step, n_cond)},
        )

    def halves(c, start, size):
        prod = [
            (spec_same * plain[c, k] + spec_cross * turned[c, k]).astype(bf16)
            for k in range(start, start + size)
        ]
        half = dot(jnp.concatenate(prod, axis=0), half_table[...]).astype(bf16)
        return [half[j * band : (j + 1) * band] for j in range(size)]

    def powers(total, pair):
        stacked = jnp.concatenate(
            [
                jnp.concatenate([h[:, :grid] for h in pair], axis=1),
                jnp.concatenate([h[:, grid:] for h in pair], axis=1),
            ],
            axis=0,
        )
        sampling = jnp.concatenate([field_table[:, :grid], field_table[:, grid:]], axis=0)
        field = dot(sampling, stacked)
        power = field[:grid] * field[:grid] + field[grid:] * field[grid:]
        for j in range(len(pair)):
            total = total + power[:, j * grid : (j + 1) * grid]
        return total

    groups = [
        (c, start, min(GROUP, kerns - start)) for c in range(conds) for start in range(0, kerns, GROUP)
    ]
    ready = [halves(*groups[i]) for i in range(min(AHEAD, len(groups)))]
    total = None
    due = []
    for i, (c, start, size) in enumerate(groups):
        if i + AHEAD < len(groups):
            ready.append(halves(*groups[i + AHEAD]))
        if start == 0:
            total = jnp.full((grid, grid), -tops[c], f32)
        half = ready[i]
        for j in range(0, size, 2):
            total = powers(total, half[j : j + 2])
        if start + size == kerns:
            level[c] = total
            for number, bunch in enumerate(bunches):
                if c == bunch[-1]:
                    due.append((i + DELAY, number))
        while due and (due[0][0] <= i or i + 1 == len(groups)):
            number = due.pop(0)[1]
            for step in range(1, n_cond):
                swap(number, step).start()

    share = high_out.shape[1]
    row_part = rise_rows[pl.ds(pl.multiple_of(me * share, share), share), :]
    row_part = jnp.concatenate([row_part[:, :grid], row_part], axis=1)
    col_part = jnp.concatenate([rise_cols[:grid], rise_cols[...]], axis=0)

    def include(bounds, values):
        high, low = high_low(jnp.concatenate(values, axis=1))
        wide = dot(row_part, jnp.concatenate([high, low, high], axis=0))
        wide = jnp.concatenate([wide[:, j * grid : (j + 1) * grid] for j in range(len(values))], axis=0)
        high, low = high_low(wide)
        blurred = dot(jnp.concatenate([high, low, high], axis=1), col_part)
        for j in range(len(values)):
            one = blurred[j * share : (j + 1) * share]
            bounds = (one, one) if bounds is None else (
                jnp.maximum(bounds[0], one),
                jnp.minimum(bounds[1], one),
            )
        return bounds

    def theirs(numbers):
        found = []
        for number in numbers:
            for step in range(1, n_cond):
                swap(number, step).wait_recv()
                found += [arrived[step - 1, c] for c in bunches[number]]
        return found

    early = theirs(range(len(bunches) - 2))
    bounds = include(None, [level[c] for c in range(conds)] + early)
    bounds = include(bounds, theirs(range(max(len(bunches) - 2, 0), len(bunches))))
    high_out[0] = bounds[0]
    low_out[0] = bounds[1]
    for step in range(1, n_cond):
        for number in range(len(bunches)):
            swap(number, step).wait_send()
    for q in range(n_cond):
        for i in range(len(around)):

            @pl.when(around[i][2] & sender)
            def _():
                halo(i, q).wait_send()


def on_device(mask, kernels, socs_weight, dose, threshold):
    core = mask.shape[1]
    conds, kerns, band, _ = kernels.shape
    n_cond = lax.axis_size("cond")
    first_table, later_table, parts = make_tables(core, band)
    share = core // n_cond
    anywhere = pl.BlockSpec(memory_space=pl.ANY)
    vmem = pl.BlockSpec(memory_space=pltpu.VMEM)
    grid = 2 * band
    out = pltpu.VMEM((1, share, core), f32)
    high, low = pl.pallas_call(
        functools.partial(body, parts),
        out_shape=(out, out),
        in_specs=[anywhere] * 7,
        out_specs=(vmem, vmem),
        scratch_shapes=[
            pltpu.SMEM(socs_weight.shape, f32),
            pltpu.SMEM(dose.shape, f32),
            pltpu.SMEM(threshold.shape, f32),
            pltpu.VMEM((core, core), bf16),
            pltpu.VMEM(kernels.shape, bf16),
            pltpu.VMEM(first_table.shape, bf16),
            pltpu.VMEM(later_table.shape, bf16),
            pltpu.VMEM((2, 3, MARGIN, 2 * band), bf16),
            pltpu.VMEM((2, 3, MARGIN, 2 * band), bf16),
            pltpu.VMEM((2, band, 2 * MARGIN), bf16),
            pltpu.VMEM((2, band, 2 * MARGIN), bf16),
            pltpu.VMEM((conds, grid, grid), f32),
            pltpu.VMEM((n_cond - 1, conds, grid, grid), f32),
            pltpu.SemaphoreType.DMA((7,)),
            pltpu.SemaphoreType.DMA((n_cond, 8)),
            pltpu.SemaphoreType.DMA((8,)),
            pltpu.SemaphoreType.DMA((n_cond - 1, min(conds, 3))),
            pltpu.SemaphoreType.DMA((n_cond - 1, min(conds, 3))),
            pltpu.VMEM(kernels.shape, f32),
            pltpu.VMEM(kernels.shape, f32),
        ],
        compiler_params=pltpu.CompilerParams(collective_id=0, has_side_effects=True),
    )(mask, kernels, socs_weight, dose, threshold, jnp.asarray(first_table), jnp.asarray(later_table))
    return jax.nn.sigmoid(high), jax.nn.sigmoid(low)


def solution(mesh):
    return jax.shard_map(
        on_device,
        mesh=mesh,
        in_specs=(
            P(("parts", "tile"), None, None),
            P("cond", None, None, None),
            P("cond", None),
            P("cond"),
            P("cond"),
        ),
        out_specs=(P(("parts", "tile"), "cond", None), P(("parts", "tile"), "cond", None)),
        check_vma=False,
    )
```

```python
import functools

import jax
import jax.numpy as jnp
import ml_dtypes
import numpy as np
from jax import lax
from jax.experimental import pallas as pl
from jax.experimental.pallas import tpu as pltpu
from jax.sharding import PartitionSpec as P

MARGIN = 64
BLUR = 8
GROUP = 4
AHEAD = 2
DELAY = 2
PIECES = 4
ORDER = (1, 4, 0, 2, 3, 6, 5, 7)

diffusion = 2.0
steepness = 8.0
bf16 = jnp.bfloat16
f32 = jnp.float32


def trig(turns, period):
    angle = 2.0 * np.pi * (turns % period) / period
    return np.cos(angle), np.sin(angle)


def split(table):
    high = table.astype(ml_dtypes.bfloat16)
    low = (table - high.astype(np.float64)).astype(ml_dtypes.bfloat16)
    return high, low


def make_tables(core, band):
    pad = core + 2 * MARGIN
    grid = 2 * band
    freq = np.arange(band) - band // 2
    cos_in, sin_in = trig(np.arange(pad)[:, None] * freq[None, :], pad)
    order = np.r_[MARGIN : MARGIN + core, 0:MARGIN, MARGIN + core : pad]
    row_table = np.concatenate([cos_in[order].T, -sin_in[order].T], axis=0)
    both = np.concatenate([cos_in, sin_in], axis=1)
    left, inner, right = both[:MARGIN], both[MARGIN : MARGIN + core], both[MARGIN + core :]
    zero = np.zeros_like(left)
    gap = np.zeros((core - 2 * MARGIN, 2 * band))
    edges = np.concatenate([right, gap, left], axis=0)
    first_table = np.concatenate(
        [row_table[:, :core], np.concatenate([inner, edges], axis=1)], axis=0
    )
    side_table = np.block([[left, zero], [zero, left], [right, zero], [zero, right]])
    cos_grid, sin_grid = trig(np.arange(grid)[:, None] * freq[None, :], grid)
    half_table = np.block([[cos_grid.T, sin_grid.T], [-sin_grid.T, cos_grid.T]])
    field_table = np.concatenate(
        [np.concatenate([cos_grid, -sin_grid], axis=1), np.concatenate([sin_grid, cos_grid], axis=1)], axis=1
    )
    pixel = np.arange(core + 2 * BLUR) + MARGIN - BLUR
    phase = pixel[:, None] / pad - np.arange(grid)[None, :] / grid
    waves = np.arange(1, band)
    interp = (1.0 + 2.0 * np.cos(2.0 * np.pi * phase[:, :, None] * waves).sum(-1)) / grid
    offset = np.arange(core + 2 * BLUR)[None, :] - np.arange(core)[:, None] - BLUR
    taps = np.exp(-(offset**2) / (2.0 * diffusion**2)) * (np.abs(offset) <= BLUR)
    reach = np.arange(-BLUR, BLUR + 1)
    taps = taps / np.exp(-(reach**2) / (2.0 * diffusion**2)).sum()
    rise = taps @ interp
    high, low = split(rise)
    rise_rows = np.concatenate([high, low], axis=1)
    rise_cols = np.concatenate([high.T, low.T], axis=0)
    outer_rows = np.concatenate([row_table[:, core:], np.zeros((2 * band, 2 * band))], axis=1)
    later = (side_table, half_table, field_table, outer_rows, rise_cols, rise_rows)
    bounds = np.cumsum([0] + [len(t) for t in later])
    later = np.concatenate([t.astype(ml_dtypes.bfloat16) for t in later], axis=0)
    return first_table.astype(ml_dtypes.bfloat16), later, [int(n) for n in bounds]


def neighbours():
    count = lax.axis_size("tile")
    columns = min(8, count // 2)
    rows = count // columns
    me = lax.axis_index("tile")
    position = lax.rem(me + columns // 2, count)
    column = lax.rem(position, columns)
    row = lax.div(position, columns)
    found = []
    for down in (-1, 0, 1):
        for right in (-1, 0, 1):
            if down == 0 and right == 0:
                continue
            flag = (row + down >= 0) & (row + down < rows)
            flag = flag & (column + right >= 0) & (column + right < columns)
            there = lax.rem(me + down * columns + right + count, count)
            found.append((down, right, flag, there))
    return found


def slot(down, right):
    return (0 if down < 0 else 1, right % 3) if down else (0 if right < 0 else 1,)


def high_low(value):
    high = value.astype(bf16)
    return high, (value - high.astype(f32)).astype(bf16)


def dot(a, b):
    return jnp.dot(a, b, preferred_element_type=f32)


def start_split(load):
    src, dst, sem = load
    rows = dst.shape[0] // PIECES
    for n in range(PIECES):
        piece = pl.ds(n * rows, rows)
        pltpu.make_async_copy(src.at[piece], dst.at[piece], sem).start()


def body(
    parts,
    mask_hbm,
    kern_hbm,
    weight_hbm,
    dose_hbm,
    threshold_hbm,
    first_hbm,
    later_hbm,
    high_out,
    low_out,
    weight,
    dose,
    threshold,
    tile,
    kern,
    first_table,
    later_table,
    rows_out,
    rows_in,
    side_out,
    side_in,
    level,
    arrived,
    halo_recv,
    swap_recv,
    plain,
    turned,
    load_sem,
    halo_send,
    swap_send,
):
    core = mask_hbm.shape[1]
    conds, kerns, band, _ = kern_hbm.shape
    grid = 2 * band
    middle_of = core // 2
    n_cond = lax.axis_size("cond")
    me = lax.axis_index("cond")
    near = n_cond - 1
    sender = me == near
    around = neighbours()
    side_table, half_table, field_table, outer_rows, rise_cols, rise_rows = (
        later_table.at[pl.ds(lo, hi - lo)] for lo, hi in zip(parts[:-1], parts[1:])
    )
    row_table = first_table.at[pl.ds(0, grid)]
    inner_table = first_table.at[pl.ds(grid, core), pl.ds(0, grid)]
    edge_table = first_table.at[pl.ds(grid, core), pl.ds(grid, grid)]

    loads = [
        (src, dst, load_sem.at[i])
        for i, (src, dst) in enumerate(
            (
                (mask_hbm.at[0], tile),
                (first_hbm, first_table),
                (kern_hbm, kern),
                (weight_hbm, weight),
                (dose_hbm, dose),
                (threshold_hbm, threshold),
                (later_hbm, later_table),
            )
        )
    ]
    for load in loads[:2]:
        start_split(load)

    barrier = pltpu.get_barrier_semaphore()
    for _, _, flag, there in around:

        @pl.when(flag)
        def _():
            pl.semaphore_signal(barrier, inc=1, device_id={"tile": there, "cond": near})

    for step in range(1, n_cond):
        pl.semaphore_signal(barrier, inc=1, device_id={"cond": lax.rem(me + step, n_cond)})
    for down, right, flag, _ in around:

        @pl.when(jnp.logical_not(flag))
        def _():
            buffer = rows_in if down else side_in
            at = slot(down, right)
            buffer[at] = jnp.zeros(buffer.shape[len(at) :], bf16)

    for load in loads[:2]:
        pltpu.make_async_copy(*load).wait()
    for load in loads[2:]:
        pltpu.make_async_copy(*load).start()
    strips = jnp.concatenate([tile[:MARGIN, :], tile[core - MARGIN :, :]], axis=0)
    middle = dot(row_table[...], tile[...]).astype(bf16)
    blocks = [
        dot(strips, inner_table[...]).astype(bf16),
        dot(strips[:, middle_of:], edge_table[middle_of:, :]).astype(bf16),
        dot(strips[:, :middle_of], edge_table[:middle_of, :]).astype(bf16),
    ]
    for at, first in ((0, 0), (1, core - MARGIN)):
        for lanes in range(3):
            rows_out[at, lanes] = blocks[lanes][at * MARGIN : (at + 1) * MARGIN]
        strip = middle[:, first : first + MARGIN]
        side_out[at] = jnp.concatenate([strip[:band], strip[band:]], axis=1)
    peers = n_cond - 1
    for _, _, flag, _ in around:
        peers = peers + jnp.where(flag & sender, n_cond, 0)
    pl.semaphore_wait(barrier, peers)

    def halo(i, q):
        down, right, flag, there = around[i]
        outgoing, incoming = (rows_out, rows_in) if down else (side_out, side_in)
        return pltpu.make_async_remote_copy(
            src_ref=outgoing.at[slot(down, right)],
            dst_ref=incoming.at[slot(-down, -right)],
            send_sem=halo_send.at[q, i],
            recv_sem=halo_recv.at[len(around) - 1 - i],
            device_id={"tile": there, "cond": q},
        )

    for i in ORDER:

        @pl.when(around[i][2] & sender)
        def _():
            for q in range(n_cond):
                halo(i, q).start()

    for load in loads[2:]:
        pltpu.make_async_copy(*load).wait()
    inner = dot(middle, inner_table[...])
    tops = []
    for c in range(conds):
        weight_sum = weight[c, 0]
        for k in range(1, kerns):
            weight_sum = weight_sum + weight[c, k]
        gain = jnp.full((8, grid), steepness * dose[c], f32) / jnp.full((8, grid), weight_sum, f32)
        tops.append(steepness * threshold[c])
        for k in range(kerns):
            root = jnp.sqrt(gain * weight[c, k])
            scaled = kern[c, k].astype(f32) * root[0:1]
            plain[c, k] = scaled
            turned[c, k] = pltpu.roll(scaled, band, 1)

    for i in ORDER:

        @pl.when(around[i][2] & sender)
        def _():
            for q in range(n_cond):
                halo(i, q).wait_send()

    for i in range(len(around)):

        @pl.when(around[i][2])
        def _():
            halo(len(around) - 1 - i, 0).wait_recv()

    outer = rows_in[...].astype(f32)
    outer = (outer[:, 0] + outer[:, 1] + outer[:, 2]).reshape(2 * MARGIN, 2 * band).astype(bf16)
    sides = dot(jnp.concatenate([side_in[0], side_in[1]], axis=1), side_table[...])
    sides = jnp.concatenate([sides[:, : 2 * band], sides[:, 2 * band :]], axis=0)
    quarters = inner + dot(outer_rows[:, : 2 * MARGIN], outer) + sides
    quarters = quarters * (1.0 / ((core + 2 * MARGIN) * band))
    turned_quarters = pltpu.roll(quarters, band, 1)
    lane = lax.broadcasted_iota(jnp.int32, (band, 2 * band), 1)
    first = lane < band
    top, bottom = quarters[:band], quarters[band:]
    top_turned, bottom_turned = turned_quarters[:band], turned_quarters[band:]
    spec_same = jnp.where(first, top + bottom_turned, top_turned + bottom)
    spec_cross = jnp.where(first, top_turned - bottom, bottom_turned - top)

    bunches = [list(range(max(conds - 2, 0)))] + [[c] for c in range(max(conds - 2, 0), conds)]
    bunches = [bunch for bunch in bunches if bunch]

    def swap(i, step):
        chosen = pl.ds(bunches[i][0], len(bunches[i]))
        return pltpu.make_async_remote_copy(
            src_ref=level.at[chosen],
            dst_ref=arrived.at[step - 1, chosen],
            send_sem=swap_send.at[step - 1, i],
            recv_sem=swap_recv.at[step - 1, i],
            device_id={"cond": lax.rem(me + step, n_cond)},
        )

    def halves(c, start, size):
        prod = [
            (spec_same * plain[c, k] + spec_cross * turned[c, k]).astype(bf16)
            for k in range(start, start + size)
        ]
        half = dot(jnp.concatenate(prod, axis=0), half_table[...]).astype(bf16)
        return [half[j * band : (j + 1) * band] for j in range(size)]

    def powers(total, pair):
        stacked = jnp.concatenate(
            [
                jnp.concatenate([h[:, :grid] for h in pair], axis=1),
                jnp.concatenate([h[:, grid:] for h in pair], axis=1),
            ],
            axis=0,
        )
        sampling = jnp.concatenate([field_table[:, :grid], field_table[:, grid:]], axis=0)
        field = dot(sampling, stacked)
        power = field[:grid] * field[:grid] + field[grid:] * field[grid:]
        for j in range(len(pair)):
            total = total + power[:, j * grid : (j + 1) * grid]
        return total

    groups = [
        (c, start, min(GROUP, kerns - start)) for c in range(conds) for start in range(0, kerns, GROUP)
    ]
    ready = [halves(*groups[i]) for i in range(min(AHEAD, len(groups)))]
    total = None
    due = []
    for i, (c, start, size) in enumerate(groups):
        if i + AHEAD < len(groups):
            ready.append(halves(*groups[i + AHEAD]))
        if start == 0:
            total = jnp.full((grid, grid), -tops[c], f32)
        half = ready[i]
        for j in range(0, size, 2):
            total = powers(total, half[j : j + 2])
        if start + size == kerns:
            level[c] = total
            for number, bunch in enumerate(bunches):
                if c == bunch[-1]:
                    due.append((i + DELAY, number))
        while due and (due[0][0] <= i or i + 1 == len(groups)):
            number = due.pop(0)[1]
            for step in range(1, n_cond):
                swap(number, step).start()

    share = high_out.shape[1]
    row_part = rise_rows[pl.ds(pl.multiple_of(me * share, share), share), :]
    row_part = jnp.concatenate([row_part[:, :grid], row_part], axis=1)
    col_part = jnp.concatenate([rise_cols[:grid], rise_cols[...]], axis=0)

    def include(bounds, values):
        high, low = high_low(jnp.concatenate(values, axis=1))
        wide = dot(row_part, jnp.concatenate([high, low, high], axis=0))
        wide = jnp.concatenate([wide[:, j * grid : (j + 1) * grid] for j in range(len(values))], axis=0)
        high, low = high_low(wide)
        blurred = dot(jnp.concatenate([high, low, high], axis=1), col_part)
        for j in range(len(values)):
            one = blurred[j * share : (j + 1) * share]
            bounds = (one, one) if bounds is None else (
                jnp.maximum(bounds[0], one),
                jnp.minimum(bounds[1], one),
            )
        return bounds

    def theirs(numbers):
        found = []
        for number in numbers:
            for step in range(1, n_cond):
                swap(number, step).wait_recv()
                found += [arrived[step - 1, c] for c in bunches[number]]
        return found

    early = theirs(range(len(bunches) - 2))
    bounds = include(None, [level[c] for c in range(conds)] + early)
    bounds = include(bounds, theirs(range(max(len(bunches) - 2, 0), len(bunches))))
    high_out[0] = bounds[0]
    low_out[0] = bounds[1]
    for step in range(1, n_cond):
        for number in range(len(bunches)):
            swap(number, step).wait_send()


def on_device(mask, kernels, socs_weight, dose, threshold):
    core = mask.shape[1]
    conds, kerns, band, _ = kernels.shape
    n_cond = lax.axis_size("cond")
    first_table, later_table, parts = make_tables(core, band)
    share = core // n_cond
    anywhere = pl.BlockSpec(memory_space=pl.ANY)
    vmem = pl.BlockSpec(memory_space=pltpu.VMEM)
    grid = 2 * band
    out = pltpu.VMEM((1, share, core), f32)

    def scoped(*refs):
        pl.run_scoped(
            functools.partial(body, parts, *refs),
            pltpu.SemaphoreType.DMA((7,)),
            pltpu.SemaphoreType.DMA((n_cond, 8)),
            pltpu.SemaphoreType.DMA((n_cond - 1, min(conds, 3))),
        )

    high, low = pl.pallas_call(
        scoped,
        out_shape=(out, out),
        in_specs=[anywhere] * 7,
        out_specs=(vmem, vmem),
        scratch_shapes=[
            pltpu.SMEM(socs_weight.shape, f32),
            pltpu.SMEM(dose.shape, f32),
            pltpu.SMEM(threshold.shape, f32),
            pltpu.VMEM((core, core), bf16),
            pltpu.VMEM(kernels.shape, bf16),
            pltpu.VMEM(first_table.shape, bf16),
            pltpu.VMEM(later_table.shape, bf16),
            pltpu.VMEM((2, 3, MARGIN, 2 * band), bf16),
            pltpu.VMEM((2, 3, MARGIN, 2 * band), bf16),
            pltpu.VMEM((2, band, 2 * MARGIN), bf16),
            pltpu.VMEM((2, band, 2 * MARGIN), bf16),
            pltpu.VMEM((conds, grid, grid), f32),
            pltpu.VMEM((n_cond - 1, conds, grid, grid), f32),
            pltpu.SemaphoreType.DMA((8,)),
            pltpu.SemaphoreType.DMA((n_cond - 1, min(conds, 3))),
            pltpu.VMEM(kernels.shape, f32),
            pltpu.VMEM(kernels.shape, f32),
        ],
        compiler_params=pltpu.CompilerParams(collective_id=0, has_side_effects=True),
    )(mask, kernels, socs_weight, dose, threshold, jnp.asarray(first_table), jnp.asarray(later_table))
    return jax.nn.sigmoid(high), jax.nn.sigmoid(low)


def solution(mesh):
    return jax.shard_map(
        on_device,
        mesh=mesh,
        in_specs=(
            P(("parts", "tile"), None, None),
            P("cond", None, None, None),
            P("cond", None),
            P("cond"),
            P("cond"),
        ),
        out_specs=(P(("parts", "tile"), "cond", None), P(("parts", "tile"), "cond", None)),
        check_vma=False,
    )
```

```python
import functools

import jax
import jax.numpy as jnp
import ml_dtypes
import numpy as np
from jax import lax
from jax.experimental import pallas as pl
from jax.experimental.pallas import tpu as pltpu
from jax.sharding import PartitionSpec as P

MARGIN = 64
BLUR = 8
GROUP = 4
AHEAD = 2
DELAY = 2
PIECES = 8
WRITES = 8
ORDER = (1, 4, 0, 2, 3, 6, 5, 7)

diffusion = 2.0
steepness = 8.0
bf16 = jnp.bfloat16
f32 = jnp.float32


def trig(turns, period):
    angle = 2.0 * np.pi * (turns % period) / period
    return np.cos(angle), np.sin(angle)


def split(table):
    high = table.astype(ml_dtypes.bfloat16)
    low = (table - high.astype(np.float64)).astype(ml_dtypes.bfloat16)
    return high, low


def make_tables(core, band):
    pad = core + 2 * MARGIN
    grid = 2 * band
    freq = np.arange(band) - band // 2
    cos_in, sin_in = trig(np.arange(pad)[:, None] * freq[None, :], pad)
    order = np.r_[MARGIN : MARGIN + core, 0:MARGIN, MARGIN + core : pad]
    row_table = np.concatenate([cos_in[order].T, -sin_in[order].T], axis=0)
    both = np.concatenate([cos_in, sin_in], axis=1)
    left, inner, right = both[:MARGIN], both[MARGIN : MARGIN + core], both[MARGIN + core :]
    zero = np.zeros_like(left)
    gap = np.zeros((core - 2 * MARGIN, 2 * band))
    edges = np.concatenate([right, gap, left], axis=0)
    first_table = np.concatenate(
        [row_table[:, :core], np.concatenate([inner, edges], axis=1)], axis=0
    )
    side_table = np.block([[left, zero], [zero, left], [right, zero], [zero, right]])
    cos_grid, sin_grid = trig(np.arange(grid)[:, None] * freq[None, :], grid)
    half_table = np.block([[cos_grid.T, sin_grid.T], [-sin_grid.T, cos_grid.T]])
    field_table = np.concatenate(
        [np.concatenate([cos_grid, -sin_grid], axis=1), np.concatenate([sin_grid, cos_grid], axis=1)], axis=1
    )
    pixel = np.arange(core + 2 * BLUR) + MARGIN - BLUR
    phase = pixel[:, None] / pad - np.arange(grid)[None, :] / grid
    waves = np.arange(1, band)
    interp = (1.0 + 2.0 * np.cos(2.0 * np.pi * phase[:, :, None] * waves).sum(-1)) / grid
    offset = np.arange(core + 2 * BLUR)[None, :] - np.arange(core)[:, None] - BLUR
    taps = np.exp(-(offset**2) / (2.0 * diffusion**2)) * (np.abs(offset) <= BLUR)
    reach = np.arange(-BLUR, BLUR + 1)
    taps = taps / np.exp(-(reach**2) / (2.0 * diffusion**2)).sum()
    rise = taps @ interp
    high, low = split(rise)
    rise_rows = np.concatenate([high, low], axis=1)
    rise_cols = np.concatenate([high.T, low.T], axis=0)
    outer_rows = np.concatenate([row_table[:, core:], np.zeros((2 * band, 2 * band))], axis=1)
    later = (side_table, half_table, field_table, outer_rows, rise_cols, rise_rows)
    bounds = np.cumsum([0] + [len(t) for t in later])
    later = np.concatenate([t.astype(ml_dtypes.bfloat16) for t in later], axis=0)
    return first_table.astype(ml_dtypes.bfloat16), later, [int(n) for n in bounds]


def neighbours():
    count = lax.axis_size("tile")
    columns = min(8, count // 2)
    rows = count // columns
    me = lax.axis_index("tile")
    position = lax.rem(me + columns // 2, count)
    column = lax.rem(position, columns)
    row = lax.div(position, columns)
    found = []
    for down in (-1, 0, 1):
        for right in (-1, 0, 1):
            if down == 0 and right == 0:
                continue
            flag = (row + down >= 0) & (row + down < rows)
            flag = flag & (column + right >= 0) & (column + right < columns)
            there = lax.rem(me + down * columns + right + count, count)
            found.append((down, right, flag, there))
    return found


def slot(down, right):
    return (0 if down < 0 else 1, right % 3) if down else (0 if right < 0 else 1,)


def high_low(value):
    high = value.astype(bf16)
    return high, (value - high.astype(f32)).astype(bf16)


def dot(a, b):
    return jnp.dot(a, b, preferred_element_type=f32)


def start_split(load):
    src, dst, sem = load
    rows = dst.shape[0] // PIECES
    for n in range(PIECES):
        piece = pl.ds(n * rows, rows)
        pltpu.make_async_copy(src.at[piece], dst.at[piece], sem).start()


def body(
    parts,
    mask_hbm,
    kern_hbm,
    weight_hbm,
    dose_hbm,
    threshold_hbm,
    first_hbm,
    later_hbm,
    high_out,
    low_out,
    weight,
    dose,
    threshold,
    tile,
    kern,
    first_table,
    later_table,
    rows_out,
    rows_in,
    side_out,
    side_in,
    level,
    arrived,
    halo_recv,
    swap_recv,
    plain,
    turned,
    load_sem,
    halo_send,
    swap_send,
):
    core = mask_hbm.shape[1]
    conds, kerns, band, _ = kern_hbm.shape
    grid = 2 * band
    middle_of = core // 2
    n_cond = lax.axis_size("cond")
    me = lax.axis_index("cond")
    near = n_cond - 1
    around = neighbours()
    tiles = lax.axis_size("tile")
    sends = [flag & jnp.where(there <= tiles // 2, me == near, me == 0) for _, _, flag, there in around]
    caller = jnp.where(lax.axis_index("tile") <= tiles // 2, near, 0)
    side_table, half_table, field_table, outer_rows, rise_cols, rise_rows = (
        later_table.at[pl.ds(lo, hi - lo)] for lo, hi in zip(parts[:-1], parts[1:])
    )
    row_table = first_table.at[pl.ds(0, grid)]
    inner_table = first_table.at[pl.ds(grid, core), pl.ds(0, grid)]
    edge_table = first_table.at[pl.ds(grid, core), pl.ds(grid, grid)]

    loads = [
        (src, dst, load_sem.at[i])
        for i, (src, dst) in enumerate(
            (
                (mask_hbm.at[0], tile),
                (first_hbm, first_table),
                (kern_hbm, kern),
                (weight_hbm, weight),
                (dose_hbm, dose),
                (threshold_hbm, threshold),
                (later_hbm, later_table),
            )
        )
    ]
    for load in loads[:2]:
        start_split(load)

    barrier = pltpu.get_barrier_semaphore()
    for i in reversed(range(len(around))):
        _, _, flag, there = around[i]

        @pl.when(flag)
        def _():
            pl.semaphore_signal(barrier, inc=1, device_id={"tile": there, "cond": caller})

    for step in range(1, n_cond):
        pl.semaphore_signal(barrier, inc=1, device_id={"cond": lax.rem(me + step, n_cond)})
    for down, right, flag, _ in around:

        @pl.when(jnp.logical_not(flag))
        def _():
            buffer = rows_in if down else side_in
            at = slot(down, right)
            buffer[at] = jnp.zeros(buffer.shape[len(at) :], bf16)

    for load in loads[:2]:
        pltpu.make_async_copy(*load).wait()
    for load in loads[2:]:
        pltpu.make_async_copy(*load).start()
    strips = jnp.concatenate([tile[:MARGIN, :], tile[core - MARGIN :, :]], axis=0)
    middle = dot(row_table[...], tile[...]).astype(bf16)
    blocks = [
        dot(strips, inner_table[...]).astype(bf16),
        dot(strips[:, middle_of:], edge_table[middle_of:, :]).astype(bf16),
        dot(strips[:, :middle_of], edge_table[:middle_of, :]).astype(bf16),
    ]
    for at, first in ((0, 0), (1, core - MARGIN)):
        for lanes in range(3):
            rows_out[at, lanes] = blocks[lanes][at * MARGIN : (at + 1) * MARGIN]
        strip = middle[:, first : first + MARGIN]
        side_out[at] = jnp.concatenate([strip[:band], strip[band:]], axis=1)
    peers = n_cond - 1
    for send in sends:
        peers = peers + jnp.where(send, n_cond, 0)
    pl.semaphore_wait(barrier, peers)

    def halo(i, q):
        down, right, _, there = around[i]
        outgoing, incoming = (rows_out, rows_in) if down else (side_out, side_in)
        return pltpu.make_async_remote_copy(
            src_ref=outgoing.at[slot(down, right)],
            dst_ref=incoming.at[slot(-down, -right)],
            send_sem=halo_send.at[q, i],
            recv_sem=halo_recv.at[len(around) - 1 - i],
            device_id={"tile": there, "cond": q},
        )

    for i in ORDER:

        @pl.when(sends[i])
        def _():
            for q in range(n_cond):
                halo(i, q).start()

    for load in loads[2:]:
        pltpu.make_async_copy(*load).wait()
    inner = dot(middle, inner_table[...])
    tops = []
    for c in range(conds):
        weight_sum = weight[c, 0]
        for k in range(1, kerns):
            weight_sum = weight_sum + weight[c, k]
        gain = jnp.full((8, grid), steepness * dose[c], f32) / jnp.full((8, grid), weight_sum, f32)
        tops.append(steepness * threshold[c])
        for k in range(kerns):
            root = jnp.sqrt(gain * weight[c, k])
            scaled = kern[c, k].astype(f32) * root[0:1]
            plain[c, k] = scaled
            turned[c, k] = pltpu.roll(scaled, band, 1)

    for i in ORDER:

        @pl.when(sends[i])
        def _():
            for q in range(n_cond):
                halo(i, q).wait_send()

    for i in range(len(around)):

        @pl.when(around[i][2])
        def _():
            halo(len(around) - 1 - i, 0).wait_recv()

    outer = rows_in[...].astype(f32)
    outer = (outer[:, 0] + outer[:, 1] + outer[:, 2]).reshape(2 * MARGIN, 2 * band).astype(bf16)
    sides = dot(jnp.concatenate([side_in[0], side_in[1]], axis=1), side_table[...])
    sides = jnp.concatenate([sides[:, : 2 * band], sides[:, 2 * band :]], axis=0)
    quarters = inner + dot(outer_rows[:, : 2 * MARGIN], outer) + sides
    quarters = quarters * (1.0 / ((core + 2 * MARGIN) * band))
    turned_quarters = pltpu.roll(quarters, band, 1)
    lane = lax.broadcasted_iota(jnp.int32, (band, 2 * band), 1)
    first = lane < band
    top, bottom = quarters[:band], quarters[band:]
    top_turned, bottom_turned = turned_quarters[:band], turned_quarters[band:]
    spec_same = jnp.where(first, top + bottom_turned, top_turned + bottom)
    spec_cross = jnp.where(first, top_turned - bottom, bottom_turned - top)

    bunches = [list(range(max(conds - 2, 0)))] + [[c] for c in range(max(conds - 2, 0), conds)]
    bunches = [bunch for bunch in bunches if bunch]

    def swap(i, step):
        chosen = pl.ds(bunches[i][0], len(bunches[i]))
        return pltpu.make_async_remote_copy(
            src_ref=level.at[chosen],
            dst_ref=arrived.at[step - 1, chosen],
            send_sem=swap_send.at[step - 1, i],
            recv_sem=swap_recv.at[step - 1, i],
            device_id={"cond": lax.rem(me + step, n_cond)},
        )

    def halves(c, start, size):
        prod = [
            (spec_same * plain[c, k] + spec_cross * turned[c, k]).astype(bf16)
            for k in range(start, start + size)
        ]
        half = dot(jnp.concatenate(prod, axis=0), half_table[...]).astype(bf16)
        return [half[j * band : (j + 1) * band] for j in range(size)]

    def powers(total, pair):
        stacked = jnp.concatenate(
            [
                jnp.concatenate([h[:, :grid] for h in pair], axis=1),
                jnp.concatenate([h[:, grid:] for h in pair], axis=1),
            ],
            axis=0,
        )
        sampling = jnp.concatenate([field_table[:, :grid], field_table[:, grid:]], axis=0)
        field = dot(sampling, stacked)
        power = field[:grid] * field[:grid] + field[grid:] * field[grid:]
        for j in range(len(pair)):
            total = total + power[:, j * grid : (j + 1) * grid]
        return total

    groups = [
        (c, start, min(GROUP, kerns - start)) for c in range(conds) for start in range(0, kerns, GROUP)
    ]
    ready = [halves(*groups[i]) for i in range(min(AHEAD, len(groups)))]
    total = None
    due = []
    for i, (c, start, size) in enumerate(groups):
        if i + AHEAD < len(groups):
            ready.append(halves(*groups[i + AHEAD]))
        if start == 0:
            total = jnp.full((grid, grid), -tops[c], f32)
        half = ready[i]
        for j in range(0, size, 2):
            total = powers(total, half[j : j + 2])
        if start + size == kerns:
            level[c] = total
            for number, bunch in enumerate(bunches):
                if c == bunch[-1]:
                    due.append((i + DELAY, number))
        while due and (due[0][0] <= i or i + 1 == len(groups)):
            number = due.pop(0)[1]
            for step in range(1, n_cond):
                swap(number, step).start()

    share = high_out.shape[1]
    row_part = rise_rows[pl.ds(pl.multiple_of(me * share, share), share), :]
    row_part = jnp.concatenate([row_part[:, :grid], row_part], axis=1)
    col_part = jnp.concatenate([rise_cols[:grid], rise_cols[...]], axis=0)

    def include(bounds, values):
        high, low = high_low(jnp.concatenate(values, axis=1))
        wide = dot(row_part, jnp.concatenate([high, low, high], axis=0))
        wide = jnp.concatenate([wide[:, j * grid : (j + 1) * grid] for j in range(len(values))], axis=0)
        high, low = high_low(wide)
        blurred = dot(jnp.concatenate([high, low, high], axis=1), col_part)
        for j in range(len(values)):
            one = blurred[j * share : (j + 1) * share]
            bounds = (one, one) if bounds is None else (
                jnp.maximum(bounds[0], one),
                jnp.minimum(bounds[1], one),
            )
        return bounds

    def theirs(numbers):
        found = []
        for number in numbers:
            for step in range(1, n_cond):
                swap(number, step).wait_recv()
                found += [arrived[step - 1, c] for c in bunches[number]]
        return found

    early = theirs(range(len(bunches) - 2))
    bounds = include(None, [level[c] for c in range(conds)] + early)
    bounds = include(bounds, theirs(range(max(len(bunches) - 2, 0), len(bunches))))
    high_out[0] = bounds[0]
    low_out[0] = bounds[1]
    for step in range(1, n_cond):
        for number in range(len(bunches)):
            swap(number, step).wait_send()


def finish(high, low, high_out, low_out, staged):
    rows = high.shape[1] // WRITES

    def write(sem):
        copies = []
        for n in range(WRITES):
            piece = pl.ds(n * rows, rows)
            for which, (src, dst) in enumerate(((high, high_out), (low, low_out))):
                staged[which, piece] = jax.nn.sigmoid(src[0, piece])
                copies.append(
                    pltpu.make_async_copy(
                        staged.at[which, piece], dst.at[0, piece], sem.at[which, n]
                    )
                )
                copies[-1].start()
        for copy in copies:
            copy.wait()

    pl.run_scoped(write, pltpu.SemaphoreType.DMA((2, WRITES)))


def on_device(mask, kernels, socs_weight, dose, threshold):
    core = mask.shape[1]
    conds, kerns, band, _ = kernels.shape
    n_cond = lax.axis_size("cond")
    first_table, later_table, parts = make_tables(core, band)
    share = core // n_cond
    anywhere = pl.BlockSpec(memory_space=pl.ANY)
    vmem = pl.BlockSpec(memory_space=pltpu.VMEM)
    grid = 2 * band
    out = pltpu.VMEM((1, share, core), f32)

    def scoped(*refs):
        pl.run_scoped(
            functools.partial(body, parts, *refs),
            pltpu.SemaphoreType.DMA((7,)),
            pltpu.SemaphoreType.DMA((n_cond, 8)),
            pltpu.SemaphoreType.DMA((n_cond - 1, min(conds, 3))),
        )

    high, low = pl.pallas_call(
        scoped,
        out_shape=(out, out),
        in_specs=[anywhere] * 7,
        out_specs=(vmem, vmem),
        scratch_shapes=[
            pltpu.SMEM(socs_weight.shape, f32),
            pltpu.SMEM(dose.shape, f32),
            pltpu.SMEM(threshold.shape, f32),
            pltpu.VMEM((core, core), bf16),
            pltpu.VMEM(kernels.shape, bf16),
            pltpu.VMEM(first_table.shape, bf16),
            pltpu.VMEM(later_table.shape, bf16),
            pltpu.VMEM((2, 3, MARGIN, 2 * band), bf16),
            pltpu.VMEM((2, 3, MARGIN, 2 * band), bf16),
            pltpu.VMEM((2, band, 2 * MARGIN), bf16),
            pltpu.VMEM((2, band, 2 * MARGIN), bf16),
            pltpu.VMEM((conds, grid, grid), f32),
            pltpu.VMEM((n_cond - 1, conds, grid, grid), f32),
            pltpu.SemaphoreType.DMA((8,)),
            pltpu.SemaphoreType.DMA((n_cond - 1, min(conds, 3))),
            pltpu.VMEM(kernels.shape, f32),
            pltpu.VMEM(kernels.shape, f32),
        ],
        compiler_params=pltpu.CompilerParams(collective_id=0, has_side_effects=True),
    )(mask, kernels, socs_weight, dose, threshold, jnp.asarray(first_table), jnp.asarray(later_table))
    out = jax.ShapeDtypeStruct((1, share, core), f32)
    return pl.pallas_call(
        finish,
        out_shape=(out, out),
        in_specs=[vmem] * 2,
        out_specs=(anywhere, anywhere),
        scratch_shapes=[pltpu.VMEM((2, share, core), f32)],
    )(*(pltpu.with_memory_space_constraint(x, pltpu.VMEM) for x in (high, low)))


def solution(mesh):
    return jax.shard_map(
        on_device,
        mesh=mesh,
        in_specs=(
            P(("parts", "tile"), None, None),
            P("cond", None, None, None),
            P("cond", None),
            P("cond"),
            P("cond"),
        ),
        out_specs=(P(("parts", "tile"), "cond", None), P(("parts", "tile"), "cond", None)),
        check_vma=False,
    )
```

```python
import functools

import jax
import jax.numpy as jnp
import ml_dtypes
import numpy as np
from jax import lax
from jax.experimental import pallas as pl
from jax.experimental.pallas import tpu as pltpu
from jax.sharding import PartitionSpec as P

MARGIN = 64
BLUR = 8
GROUP = 4
AHEAD = 2
DELAY = 2
PIECES = 8
WRITES = 8
SWAPS = 1
ORDER = (1, 4, 0, 2, 3, 6, 5, 7)

diffusion = 2.0
steepness = 8.0
bf16 = jnp.bfloat16
f32 = jnp.float32


def trig(turns, period):
    angle = 2.0 * np.pi * (turns % period) / period
    return np.cos(angle), np.sin(angle)


def split(table):
    high = table.astype(ml_dtypes.bfloat16)
    low = (table - high.astype(np.float64)).astype(ml_dtypes.bfloat16)
    return high, low


def make_tables(core, band):
    pad = core + 2 * MARGIN
    grid = 2 * band
    freq = np.arange(band) - band // 2
    cos_in, sin_in = trig(np.arange(pad)[:, None] * freq[None, :], pad)
    order = np.r_[MARGIN : MARGIN + core, 0:MARGIN, MARGIN + core : pad]
    row_table = np.concatenate([cos_in[order].T, -sin_in[order].T], axis=0)
    both = np.concatenate([cos_in, sin_in], axis=1)
    left, inner, right = both[:MARGIN], both[MARGIN : MARGIN + core], both[MARGIN + core :]
    gap = np.zeros((core - 2 * MARGIN, 2 * band))
    edges = np.concatenate([right, gap, left], axis=0)
    first_table = np.concatenate(
        [row_table[:, :core], np.concatenate([inner, edges], axis=1)], axis=0
    )
    strips = []
    for strip in (left, right):
        cos, sin = strip[:, :band], strip[:, band:]
        strips.append(np.concatenate([cos, cos, sin, -sin], axis=1))
        strips.append(np.concatenate([sin, sin, -cos, cos], axis=1))
    side_table = np.concatenate(strips, axis=0)
    cos_grid, sin_grid = trig(np.arange(grid)[:, None] * freq[None, :], grid)
    half_table = np.block([[cos_grid.T, sin_grid.T], [-sin_grid.T, cos_grid.T]])
    field_table = np.concatenate(
        [np.concatenate([cos_grid, -sin_grid], axis=1), np.concatenate([sin_grid, cos_grid], axis=1)], axis=1
    )
    pixel = np.arange(core + 2 * BLUR) + MARGIN - BLUR
    phase = pixel[:, None] / pad - np.arange(grid)[None, :] / grid
    waves = np.arange(1, band)
    interp = (1.0 + 2.0 * np.cos(2.0 * np.pi * phase[:, :, None] * waves).sum(-1)) / grid
    offset = np.arange(core + 2 * BLUR)[None, :] - np.arange(core)[:, None] - BLUR
    taps = np.exp(-(offset**2) / (2.0 * diffusion**2)) * (np.abs(offset) <= BLUR)
    reach = np.arange(-BLUR, BLUR + 1)
    taps = taps / np.exp(-(reach**2) / (2.0 * diffusion**2)).sum()
    rise = taps @ interp
    high, low = split(rise)
    rise_rows = np.concatenate([high, low], axis=1)
    rise_cols = np.concatenate([high.T, low.T], axis=0)
    outer_rows = np.concatenate([row_table[:, core:], np.zeros((2 * band, 2 * band))], axis=1)
    later = (side_table, half_table, field_table, outer_rows, rise_cols, rise_rows)
    bounds = np.cumsum([0] + [len(t) for t in later])
    later = np.concatenate([t.astype(ml_dtypes.bfloat16) for t in later], axis=0)
    return first_table.astype(ml_dtypes.bfloat16), later, [int(n) for n in bounds]


def neighbours():
    count = lax.axis_size("tile")
    columns = min(8, count // 2)
    rows = count // columns
    me = lax.axis_index("tile")
    position = lax.rem(me + columns // 2, count)
    column = lax.rem(position, columns)
    row = lax.div(position, columns)
    found = []
    for down in (-1, 0, 1):
        for right in (-1, 0, 1):
            if down == 0 and right == 0:
                continue
            flag = (row + down >= 0) & (row + down < rows)
            flag = flag & (column + right >= 0) & (column + right < columns)
            there = lax.rem(me + down * columns + right + count, count)
            found.append((down, right, flag, there))
    return found


def slot(down, right):
    return (0 if down < 0 else 1, right % 3) if down else (0 if right < 0 else 1,)


def high_low(value):
    high = value.astype(bf16)
    return high, (value - high.astype(f32)).astype(bf16)


def dot(a, b):
    return jnp.dot(a, b, preferred_element_type=f32)


def start_split(load):
    src, dst, sem = load
    rows = dst.shape[0] // PIECES
    for n in range(PIECES):
        piece = pl.ds(n * rows, rows)
        pltpu.make_async_copy(src.at[piece], dst.at[piece], sem).start()


def body(
    parts,
    mask_hbm,
    kern_hbm,
    weight_hbm,
    dose_hbm,
    threshold_hbm,
    first_hbm,
    later_hbm,
    high_out,
    low_out,
    weight,
    dose,
    threshold,
    tile,
    kern,
    first_table,
    later_table,
    rows_out,
    rows_in,
    side_out,
    side_in,
    level,
    arrived,
    halo_recv,
    swap_recv,
    plain,
    turned,
    load_sem,
    halo_send,
    swap_send,
):
    core = mask_hbm.shape[1]
    conds, kerns, band, _ = kern_hbm.shape
    grid = 2 * band
    side_table, half_table, field_table, outer_rows, rise_cols, rise_rows = (
        later_table.at[pl.ds(lo, hi - lo)] for lo, hi in zip(parts[:-1], parts[1:])
    )
    row_table = first_table.at[pl.ds(0, grid)]
    inner_table = first_table.at[pl.ds(grid, core), pl.ds(0, grid)]
    edge_table = first_table.at[pl.ds(grid, core), pl.ds(grid, grid)]

    loads = [
        (src, dst, load_sem.at[i])
        for i, (src, dst) in enumerate(
            (
                (mask_hbm.at[0], tile),
                (first_hbm.at[pl.ds(0, grid)], first_table.at[pl.ds(0, grid)]),
                (first_hbm.at[pl.ds(grid, core)], first_table.at[pl.ds(grid, core)]),
                (kern_hbm, kern),
                (weight_hbm, weight),
                (dose_hbm, dose),
                (threshold_hbm, threshold),
                (later_hbm, later_table),
            )
        )
    ]
    for load in loads[:3]:
        start_split(load)

    middle_of = core // 2
    n_cond = lax.axis_size("cond")
    me = lax.axis_index("cond")
    near = n_cond - 1
    around = neighbours()
    tiles = lax.axis_size("tile")
    sends = [flag & jnp.where(there <= tiles // 2 + 1, me == near, me == 0) for _, _, flag, there in around]
    caller = jnp.where(lax.axis_index("tile") <= tiles // 2 + 1, near, 0)
    barrier = pltpu.get_barrier_semaphore()
    for i in reversed(range(len(around))):
        _, _, flag, there = around[i]

        @pl.when(flag)
        def _():
            pl.semaphore_signal(barrier, inc=1, device_id={"tile": there, "cond": caller})

    for step in range(1, n_cond):
        pl.semaphore_signal(barrier, inc=1, device_id={"cond": lax.rem(me + step, n_cond)})
    for down, right, flag, _ in around:

        @pl.when(jnp.logical_not(flag))
        def _():
            buffer = rows_in if down else side_in
            at = slot(down, right)
            buffer[at] = jnp.zeros(buffer.shape[len(at) :], bf16)

    for load in loads[:2]:
        pltpu.make_async_copy(*load).wait()
    for load in loads[3:]:
        pltpu.make_async_copy(*load).start()
    lane = lax.broadcasted_iota(jnp.int32, (band, 2 * band), 1)
    first = lane < band
    wide_first = lax.broadcasted_iota(jnp.int32, (core, grid), 1) < band
    edges = jnp.where(wide_first, tile[:, :grid], tile[:, core - grid :])
    edges = dot(row_table[...], edges)
    turned_edges = pltpu.roll(edges, band, 1)
    side_out[0] = jnp.where(first, edges[:band], turned_edges[band:]).astype(bf16)
    side_out[1] = jnp.where(first, turned_edges[:band], edges[band:]).astype(bf16)
    peers = n_cond - 1
    for send in sends:
        peers = peers + jnp.where(send, n_cond, 0)
    pl.semaphore_wait(barrier, peers)

    def halo(i, q):
        down, right, _, there = around[i]
        outgoing, incoming = (rows_out, rows_in) if down else (side_out, side_in)
        return pltpu.make_async_remote_copy(
            src_ref=outgoing.at[slot(down, right)],
            dst_ref=incoming.at[slot(-down, -right)],
            send_sem=halo_send.at[q, i],
            recv_sem=halo_recv.at[len(around) - 1 - i],
            device_id={"tile": there, "cond": q},
        )

    def depart(numbers):
        for i in numbers:

            @pl.when(sends[i])
            def _():
                for q in range(n_cond):
                    halo(i, q).start()

    depart(i for i in ORDER if not around[i][0])
    pltpu.make_async_copy(*loads[2]).wait()
    strips = jnp.concatenate([tile[:MARGIN, :], tile[core - MARGIN :, :]], axis=0)
    blocks = [
        dot(strips, inner_table[...]).astype(bf16),
        dot(strips[:, middle_of:], edge_table[middle_of:, :]).astype(bf16),
        dot(strips[:, :middle_of], edge_table[:middle_of, :]).astype(bf16),
    ]
    for at in range(2):
        for lanes in range(3):
            rows_out[at, lanes] = blocks[lanes][at * MARGIN : (at + 1) * MARGIN]
    depart(i for i in ORDER if around[i][0])

    for load in loads[3:]:
        pltpu.make_async_copy(*load).wait()
    middle = dot(row_table[...], tile[...]).astype(bf16)
    inner = dot(middle, inner_table[...])
    tops = []
    for c in range(conds):
        weight_sum = weight[c, 0]
        for k in range(1, kerns):
            weight_sum = weight_sum + weight[c, k]
        gain = jnp.full((8, grid), steepness * dose[c], f32) / jnp.full((8, grid), weight_sum, f32)
        tops.append(steepness * threshold[c])
        for k in range(kerns):
            root = jnp.sqrt(gain * weight[c, k]) * (1.0 / ((core + 2 * MARGIN) * band))
            scaled = kern[c, k].astype(f32) * root[0:1]
            plain[c, k] = scaled
            turned[c, k] = pltpu.roll(scaled, band, 1)

    def arrive(numbers):
        for i in numbers:

            @pl.when(around[i][2])
            def _():
                halo(len(around) - 1 - i, 0).wait_recv()

    arrive(i for i in range(len(around)) if around[i][0])
    outer = rows_in[...].astype(f32)
    outer = (outer[:, 0] + outer[:, 1] + outer[:, 2]).reshape(2 * MARGIN, 2 * band).astype(bf16)
    quarters = inner + dot(outer_rows[:, : 2 * MARGIN], outer)
    turned_quarters = pltpu.roll(quarters, band, 1)
    top, bottom = quarters[:band], quarters[band:]
    top_turned, bottom_turned = turned_quarters[:band], turned_quarters[band:]
    spec_same = jnp.where(first, top + bottom_turned, top_turned + bottom)
    spec_cross = jnp.where(first, top_turned - bottom, bottom_turned - top)
    arrive(i for i in range(len(around)) if not around[i][0])
    sides = dot(jnp.concatenate([side_in[0], side_in[1]], axis=1), side_table[...])
    spec_same = spec_same + sides[:, : 2 * band]
    spec_cross = spec_cross + sides[:, 2 * band :]

    bunches = [list(range(max(conds - 2, 0)))] + [[c] for c in range(max(conds - 2, 0), conds)]
    bunches = [bunch for bunch in bunches if bunch]

    def swap(i, step, rows=pl.ds(0, grid)):
        chosen = pl.ds(bunches[i][0], len(bunches[i]))
        return pltpu.make_async_remote_copy(
            src_ref=level.at[chosen, rows],
            dst_ref=arrived.at[step - 1, chosen, rows],
            send_sem=swap_send.at[step - 1, i],
            recv_sem=swap_recv.at[step - 1, i],
            device_id={"cond": lax.rem(me + step, n_cond)},
        )

    def halves(c, start, size):
        prod = [
            (spec_same * plain[c, k] + spec_cross * turned[c, k]).astype(bf16)
            for k in range(start, start + size)
        ]
        half = dot(jnp.concatenate(prod, axis=0), half_table[...]).astype(bf16)
        return [half[j * band : (j + 1) * band] for j in range(size)]

    def powers(total, pair):
        stacked = jnp.concatenate(
            [
                jnp.concatenate([h[:, :grid] for h in pair], axis=1),
                jnp.concatenate([h[:, grid:] for h in pair], axis=1),
            ],
            axis=0,
        )
        sampling = jnp.concatenate([field_table[:, :grid], field_table[:, grid:]], axis=0)
        field = dot(sampling, stacked)
        power = field[:grid] * field[:grid] + field[grid:] * field[grid:]
        for j in range(len(pair)):
            total = total + power[:, j * grid : (j + 1) * grid]
        return total

    groups = [
        (c, start, min(GROUP, kerns - start)) for c in range(conds) for start in range(0, kerns, GROUP)
    ]
    ready = [halves(*groups[i]) for i in range(min(AHEAD, len(groups)))]
    total = None
    due = []
    for i, (c, start, size) in enumerate(groups):
        if i + AHEAD < len(groups):
            ready.append(halves(*groups[i + AHEAD]))
        if start == 0:
            total = jnp.full((grid, grid), -tops[c], f32)
        half = ready[i]
        for j in range(0, size, 2):
            total = powers(total, half[j : j + 2])
        if start + size == kerns:
            level[c] = total
            for number, bunch in enumerate(bunches):
                if c == bunch[-1]:
                    due.append((i + DELAY, number))
        while due and (due[0][0] <= i or i + 1 == len(groups)):
            number = due.pop(0)[1]
            for step in range(1, n_cond):
                for n in range(SWAPS):
                    swap(number, step, pl.ds(n * (grid // SWAPS), grid // SWAPS)).start()

    share = high_out.shape[1]
    row_part = rise_rows[pl.ds(pl.multiple_of(me * share, share), share), :]
    row_part = jnp.concatenate([row_part[:, :grid], row_part], axis=1)
    col_part = jnp.concatenate([rise_cols[:grid], rise_cols[...]], axis=0)

    def include(bounds, values):
        high, low = high_low(jnp.concatenate(values, axis=1))
        wide = dot(row_part, jnp.concatenate([high, low, high], axis=0))
        wide = jnp.concatenate([wide[:, j * grid : (j + 1) * grid] for j in range(len(values))], axis=0)
        high, low = high_low(wide)
        blurred = dot(jnp.concatenate([high, low, high], axis=1), col_part)
        for j in range(len(values)):
            one = blurred[j * share : (j + 1) * share]
            bounds = (one, one) if bounds is None else (
                jnp.maximum(bounds[0], one),
                jnp.minimum(bounds[1], one),
            )
        return bounds

    def theirs(numbers):
        found = []
        for number in numbers:
            for step in range(1, n_cond):
                swap(number, step).wait_recv()
                found += [arrived[step - 1, c] for c in bunches[number]]
        return found

    early = theirs(range(len(bunches) - 2))
    bounds = include(None, [level[c] for c in range(conds)] + early)
    for i in ORDER:

        @pl.when(sends[i])
        def _():
            for q in range(n_cond):
                halo(i, q).wait_send()

    bounds = include(bounds, theirs(range(max(len(bunches) - 2, 0), len(bunches))))
    high_out[0] = bounds[0]
    low_out[0] = bounds[1]
    for step in range(1, n_cond):
        for number in range(len(bunches)):
            swap(number, step).wait_send()


def finish(high, low, high_out, low_out, staged):
    rows = high.shape[1] // WRITES

    def write(sem):
        copies = []
        for n in range(WRITES):
            piece = pl.ds(n * rows, rows)
            for which, (src, dst) in enumerate(((high, high_out), (low, low_out))):
                staged[which, piece] = jax.nn.sigmoid(src[0, piece])
                copies.append(
                    pltpu.make_async_copy(
                        staged.at[which, piece], dst.at[0, piece], sem.at[which, n]
                    )
                )
                copies[-1].start()
        for copy in copies:
            copy.wait()

    pl.run_scoped(write, pltpu.SemaphoreType.DMA((2, WRITES)))


def on_device(mask, kernels, socs_weight, dose, threshold):
    core = mask.shape[1]
    conds, kerns, band, _ = kernels.shape
    n_cond = lax.axis_size("cond")
    first_table, later_table, parts = make_tables(core, band)
    share = core // n_cond
    anywhere = pl.BlockSpec(memory_space=pl.ANY)
    vmem = pl.BlockSpec(memory_space=pltpu.VMEM)
    grid = 2 * band
    out = pltpu.VMEM((1, share, core), f32)

    def scoped(*refs):
        pl.run_scoped(
            functools.partial(body, parts, *refs),
            pltpu.SemaphoreType.DMA((8,)),
            pltpu.SemaphoreType.DMA((n_cond, 8)),
            pltpu.SemaphoreType.DMA((n_cond - 1, min(conds, 3))),
        )

    high, low = pl.pallas_call(
        scoped,
        out_shape=(out, out),
        in_specs=[anywhere] * 7,
        out_specs=(vmem, vmem),
        scratch_shapes=[
            pltpu.SMEM(socs_weight.shape, f32),
            pltpu.SMEM(dose.shape, f32),
            pltpu.SMEM(threshold.shape, f32),
            pltpu.VMEM((core, core), bf16),
            pltpu.VMEM(kernels.shape, bf16),
            pltpu.VMEM(first_table.shape, bf16),
            pltpu.VMEM(later_table.shape, bf16),
            pltpu.VMEM((2, 3, MARGIN, 2 * band), bf16),
            pltpu.VMEM((2, 3, MARGIN, 2 * band), bf16),
            pltpu.VMEM((2, band, 2 * MARGIN), bf16),
            pltpu.VMEM((2, band, 2 * MARGIN), bf16),
            pltpu.VMEM((conds, grid, grid), f32),
            pltpu.VMEM((n_cond - 1, conds, grid, grid), f32),
            pltpu.SemaphoreType.DMA((8,)),
            pltpu.SemaphoreType.DMA((n_cond - 1, min(conds, 3))),
            pltpu.VMEM(kernels.shape, f32),
            pltpu.VMEM(kernels.shape, f32),
        ],
        compiler_params=pltpu.CompilerParams(collective_id=0, has_side_effects=True),
    )(mask, kernels, socs_weight, dose, threshold, jnp.asarray(first_table), jnp.asarray(later_table))
    out = jax.ShapeDtypeStruct((1, share, core), f32)
    return pl.pallas_call(
        finish,
        out_shape=(out, out),
        in_specs=[vmem] * 2,
        out_specs=(anywhere, anywhere),
        scratch_shapes=[pltpu.VMEM((2, share, core), f32)],
    )(*(pltpu.with_memory_space_constraint(x, pltpu.VMEM) for x in (high, low)))


def solution(mesh):
    return jax.shard_map(
        on_device,
        mesh=mesh,
        in_specs=(
            P(("parts", "tile"), None, None),
            P("cond", None, None, None),
            P("cond", None),
            P("cond"),
            P("cond"),
        ),
        out_specs=(P(("parts", "tile"), "cond", None), P(("parts", "tile"), "cond", None)),
        check_vma=False,
    )
```

```python
import functools

import jax
import jax.numpy as jnp
import ml_dtypes
import numpy as np
from jax import lax
from jax.experimental import pallas as pl
from jax.experimental.pallas import tpu as pltpu
from jax.sharding import PartitionSpec as P

MARGIN = 64
BLUR = 8
GROUP = 4
AHEAD = 3
DELAY = 2
PIECES = 8
WRITES = 8
SWAPS = 1
ORDER = (4, 3, 0, 1, 2, 7, 6, 5)

diffusion = 2.0
steepness = 8.0
bf16 = jnp.bfloat16
f32 = jnp.float32


def trig(turns, period):
    angle = 2.0 * np.pi * (turns % period) / period
    return np.cos(angle), np.sin(angle)


def split(table):
    high = table.astype(ml_dtypes.bfloat16)
    low = (table - high.astype(np.float64)).astype(ml_dtypes.bfloat16)
    return high, low


def make_tables(core, band):
    pad = core + 2 * MARGIN
    grid = 2 * band
    freq = np.arange(band) - band // 2
    cos_in, sin_in = trig(np.arange(pad)[:, None] * freq[None, :], pad)
    order = np.r_[MARGIN : MARGIN + core, 0:MARGIN, MARGIN + core : pad]
    row_table = np.concatenate([cos_in[order].T, -sin_in[order].T], axis=0)
    both = np.concatenate([cos_in, sin_in], axis=1)
    left, inner, right = both[:MARGIN], both[MARGIN : MARGIN + core], both[MARGIN + core :]
    gap = np.zeros((core - 2 * MARGIN, 2 * band))
    edges = np.concatenate([right, gap, left], axis=0)
    first_table = np.concatenate(
        [row_table[:, :core], np.concatenate([inner, edges], axis=1)], axis=0
    )
    strips = []
    for strip in (left, right):
        cos, sin = strip[:, :band], strip[:, band:]
        strips.append(np.concatenate([cos, cos, sin, -sin], axis=1))
        strips.append(np.concatenate([sin, sin, -cos, cos], axis=1))
    side_table = np.concatenate(strips, axis=0)
    cos_grid, sin_grid = trig(np.arange(grid)[:, None] * freq[None, :], grid)
    half_table = np.block([[cos_grid.T, sin_grid.T], [-sin_grid.T, cos_grid.T]])
    field_table = np.concatenate(
        [np.concatenate([cos_grid, -sin_grid], axis=1), np.concatenate([sin_grid, cos_grid], axis=1)], axis=1
    )
    pixel = np.arange(core + 2 * BLUR) + MARGIN - BLUR
    phase = pixel[:, None] / pad - np.arange(grid)[None, :] / grid
    waves = np.arange(1, band)
    interp = (1.0 + 2.0 * np.cos(2.0 * np.pi * phase[:, :, None] * waves).sum(-1)) / grid
    offset = np.arange(core + 2 * BLUR)[None, :] - np.arange(core)[:, None] - BLUR
    taps = np.exp(-(offset**2) / (2.0 * diffusion**2)) * (np.abs(offset) <= BLUR)
    reach = np.arange(-BLUR, BLUR + 1)
    taps = taps / np.exp(-(reach**2) / (2.0 * diffusion**2)).sum()
    rise = taps @ interp
    high, low = split(rise)
    rise_rows = np.concatenate([high, low], axis=1)
    rise_cols = np.concatenate([high.T, low.T], axis=0)
    outer_rows = np.concatenate([row_table[:, core:], np.zeros((2 * band, 2 * band))], axis=1)
    later = (side_table, half_table, field_table, outer_rows, rise_cols, rise_rows)
    bounds = np.cumsum([0] + [len(t) for t in later])
    later = np.concatenate([t.astype(ml_dtypes.bfloat16) for t in later], axis=0)
    return first_table.astype(ml_dtypes.bfloat16), later, [int(n) for n in bounds]


def neighbours():
    count = lax.axis_size("tile")
    columns = min(8, count // 2)
    rows = count // columns
    me = lax.axis_index("tile")
    position = lax.rem(me + columns // 2, count)
    column = lax.rem(position, columns)
    row = lax.div(position, columns)
    found = []
    for down in (-1, 0, 1):
        for right in (-1, 0, 1):
            if down == 0 and right == 0:
                continue
            flag = (row + down >= 0) & (row + down < rows)
            flag = flag & (column + right >= 0) & (column + right < columns)
            there = lax.rem(me + down * columns + right + count, count)
            found.append((down, right, flag, there))
    return found


def slot(down, right):
    return (0 if down < 0 else 1, right % 3) if down else (0 if right < 0 else 1,)


def high_low(value):
    high = value.astype(bf16)
    return high, (value - high.astype(f32)).astype(bf16)


def dot(a, b):
    return jnp.dot(a, b, preferred_element_type=f32)


def start_split(load):
    src, dst, sem = load
    rows = dst.shape[0] // PIECES
    for n in range(PIECES):
        piece = pl.ds(n * rows, rows)
        pltpu.make_async_copy(src.at[piece], dst.at[piece], sem).start()


def body(
    parts,
    mask_hbm,
    kern_hbm,
    weight_hbm,
    dose_hbm,
    threshold_hbm,
    first_hbm,
    later_hbm,
    high_out,
    low_out,
    weight,
    dose,
    threshold,
    tile,
    kern,
    first_table,
    later_table,
    rows_out,
    rows_in,
    side_out,
    side_in,
    level,
    arrived,
    halo_recv,
    swap_recv,
    forward_recv,
    outer,
    spec,
    plain,
    turned,
    load_sem,
    halo_send,
    swap_send,
    forward_send,
):
    core = mask_hbm.shape[1]
    conds, kerns, band, _ = kern_hbm.shape
    grid = 2 * band
    side_table, half_table, field_table, outer_rows, rise_cols, rise_rows = (
        later_table.at[pl.ds(lo, hi - lo)] for lo, hi in zip(parts[:-1], parts[1:])
    )
    row_table = first_table.at[pl.ds(0, grid)]
    inner_table = first_table.at[pl.ds(grid, core), pl.ds(0, grid)]
    edge_table = first_table.at[pl.ds(grid, core), pl.ds(grid, grid)]

    loads = [
        (src, dst, load_sem.at[i])
        for i, (src, dst) in enumerate(
            (
                (mask_hbm.at[0], tile),
                (first_hbm.at[pl.ds(0, grid)], first_table.at[pl.ds(0, grid)]),
                (first_hbm.at[pl.ds(grid, core)], first_table.at[pl.ds(grid, core)]),
                (kern_hbm, kern),
                (weight_hbm, weight),
                (dose_hbm, dose),
                (threshold_hbm, threshold),
                (later_hbm, later_table),
            )
        )
    ]
    for load in loads[:3]:
        start_split(load)

    middle_of = core // 2
    n_cond = lax.axis_size("cond")
    me = lax.axis_index("cond")
    near = n_cond - 1
    around = neighbours()
    tiles = lax.axis_size("tile")
    sends = [flag & jnp.where(there <= tiles // 2 + 1, me == near, me == 0) for _, _, flag, there in around]

    def targets(i):
        return (near,) if around[i][0] else tuple(range(n_cond))

    caller = jnp.where(lax.axis_index("tile") <= tiles // 2 + 1, near, 0)
    barrier = pltpu.get_barrier_semaphore()
    for i in reversed(range(len(around))):
        down, _, flag, there = around[i]

        @pl.when(flag & (me == near) if down else flag)
        def _():
            pl.semaphore_signal(barrier, inc=1, device_id={"tile": there, "cond": caller})

    for step in range(1, n_cond):
        pl.semaphore_signal(barrier, inc=1, device_id={"cond": lax.rem(me + step, n_cond)})
    for down, right, flag, _ in around:

        @pl.when(jnp.logical_not(flag))
        def _():
            buffer = rows_in if down else side_in
            at = slot(down, right)
            buffer[at] = jnp.zeros(buffer.shape[len(at) :], bf16)

    for load in loads[:2]:
        pltpu.make_async_copy(*load).wait()
    for load in loads[3:]:
        pltpu.make_async_copy(*load).start()
    lane = lax.broadcasted_iota(jnp.int32, (band, 2 * band), 1)
    first = lane < band
    wide_first = lax.broadcasted_iota(jnp.int32, (core, grid), 1) < band
    edges = jnp.where(wide_first, tile[:, :grid], tile[:, core - grid :])
    edges = dot(row_table[...], edges)
    turned_edges = pltpu.roll(edges, band, 1)
    side_out[0] = jnp.where(first, edges[:band], turned_edges[band:]).astype(bf16)
    side_out[1] = jnp.where(first, turned_edges[:band], edges[band:]).astype(bf16)
    peers = n_cond - 1
    for i, send in enumerate(sends):
        peers = peers + jnp.where(send, len(targets(i)), 0)
    pl.semaphore_wait(barrier, peers)

    def halo(i, q):
        down, right, _, there = around[i]
        outgoing, incoming = (rows_out, rows_in) if down else (side_out, side_in)
        return pltpu.make_async_remote_copy(
            src_ref=outgoing.at[slot(down, right)],
            dst_ref=incoming.at[slot(-down, -right)],
            send_sem=halo_send.at[q, i],
            recv_sem=halo_recv.at[len(around) - 1 - i],
            device_id={"tile": there, "cond": q},
        )

    def depart(numbers):
        for i in numbers:

            @pl.when(sends[i])
            def _():
                for q in targets(i):
                    halo(i, q).start()

    depart(i for i in ORDER if not around[i][0])
    pltpu.make_async_copy(*loads[2]).wait()
    strips = jnp.concatenate([tile[:MARGIN, :], tile[core - MARGIN :, :]], axis=0)
    blocks = [
        dot(strips, inner_table[...]).astype(bf16),
        dot(strips[:, middle_of:], edge_table[middle_of:, :]).astype(bf16),
        dot(strips[:, :middle_of], edge_table[:middle_of, :]).astype(bf16),
    ]
    for at in range(2):
        for lanes in range(3):
            rows_out[at, lanes] = blocks[lanes][at * MARGIN : (at + 1) * MARGIN]
    depart(i for i in ORDER if around[i][0])

    for load in loads[3:]:
        pltpu.make_async_copy(*load).wait()
    middle = dot(row_table[...], tile[...]).astype(bf16)
    inner = dot(middle, inner_table[...])
    tops = []
    for c in range(conds):
        weight_sum = weight[c, 0]
        for k in range(1, kerns):
            weight_sum = weight_sum + weight[c, k]
        gain = jnp.full((8, grid), steepness * dose[c], f32) / jnp.full((8, grid), weight_sum, f32)
        tops.append(steepness * threshold[c])
        for k in range(kerns):
            root = jnp.sqrt(gain * weight[c, k]) * (1.0 / ((core + 2 * MARGIN) * band))
            scaled = kern[c, k].astype(f32) * root[0:1]
            plain[c, k] = scaled
            turned[c, k] = pltpu.roll(scaled, band, 1)

    def arrive(numbers):
        for i in numbers:

            @pl.when(around[i][2])
            def _():
                halo(len(around) - 1 - i, 0).wait_recv()

    def forward(q):
        return pltpu.make_async_remote_copy(
            src_ref=outer,
            dst_ref=outer,
            send_sem=forward_send.at[q],
            recv_sem=forward_recv,
            device_id={"cond": q},
        )

    def from_rows():
        quarters = inner + dot(outer_rows[:, : 2 * MARGIN], outer[...])
        turned_quarters = pltpu.roll(quarters, band, 1)
        top, bottom = quarters[:band], quarters[band:]
        top_turned, bottom_turned = turned_quarters[:band], turned_quarters[band:]
        same = jnp.where(first, top + bottom_turned, top_turned + bottom)
        cross = jnp.where(first, top_turned - bottom, bottom_turned - top)
        return same, cross

    def from_sides(same, cross):
        sides = dot(jnp.concatenate([side_in[0], side_in[1]], axis=1), side_table[...])
        spec[0] = same + sides[:, : 2 * band]
        spec[1] = cross + sides[:, 2 * band :]

    beside = [i for i in range(len(around)) if not around[i][0]]

    @pl.when(me == near)
    def _():
        arrive(i for i in range(len(around)) if around[i][0])
        rows = rows_in[...].astype(f32)
        rows = rows[:, 0] + rows[:, 1] + rows[:, 2]
        outer[...] = rows.reshape(2 * MARGIN, 2 * band).astype(bf16)
        for q in range(near):
            forward(q).start()
        same, cross = from_rows()
        arrive(beside)
        from_sides(same, cross)

    @pl.when(me != near)
    def _():
        arrive(beside)
        forward(0).wait_recv()
        from_sides(*from_rows())

    spec_same, spec_cross = spec[0], spec[1]

    bunches = [list(range(max(conds - 2, 0)))] + [[c] for c in range(max(conds - 2, 0), conds)]
    bunches = [bunch for bunch in bunches if bunch]

    def swap(i, step, rows=pl.ds(0, grid)):
        chosen = pl.ds(bunches[i][0], len(bunches[i]))
        return pltpu.make_async_remote_copy(
            src_ref=level.at[chosen, rows],
            dst_ref=arrived.at[step - 1, chosen, rows],
            send_sem=swap_send.at[step - 1, i],
            recv_sem=swap_recv.at[step - 1, i],
            device_id={"cond": lax.rem(me + step, n_cond)},
        )

    def halves(c, start, size):
        prod = [
            (spec_same * plain[c, k] + spec_cross * turned[c, k]).astype(bf16)
            for k in range(start, start + size)
        ]
        half = dot(jnp.concatenate(prod, axis=0), half_table[...]).astype(bf16)
        return [half[j * band : (j + 1) * band] for j in range(size)]

    def powers(total, pair):
        stacked = jnp.concatenate(
            [
                jnp.concatenate([h[:, :grid] for h in pair], axis=1),
                jnp.concatenate([h[:, grid:] for h in pair], axis=1),
            ],
            axis=0,
        )
        sampling = jnp.concatenate([field_table[:, :grid], field_table[:, grid:]], axis=0)
        field = dot(sampling, stacked)
        power = field[:grid] * field[:grid] + field[grid:] * field[grid:]
        for j in range(len(pair)):
            total = total + power[:, j * grid : (j + 1) * grid]
        return total

    groups = [
        (c, start, min(GROUP, kerns - start)) for c in range(conds) for start in range(0, kerns, GROUP)
    ]
    ready = [halves(*groups[i]) for i in range(min(AHEAD, len(groups)))]
    total = None
    due = []
    for i, (c, start, size) in enumerate(groups):
        if i + AHEAD < len(groups):
            ready.append(halves(*groups[i + AHEAD]))
        if start == 0:
            total = jnp.full((grid, grid), -tops[c], f32)
        half = ready[i]
        for j in range(0, size, 2):
            total = powers(total, half[j : j + 2])
        if start + size == kerns:
            level[c] = total
            for number, bunch in enumerate(bunches):
                if c == bunch[-1]:
                    due.append((i + DELAY, number))
        while due and (due[0][0] <= i or i + 1 == len(groups)):
            number = due.pop(0)[1]
            for step in range(1, n_cond):
                for n in range(SWAPS):
                    swap(number, step, pl.ds(n * (grid // SWAPS), grid // SWAPS)).start()

    share = high_out.shape[1]
    row_part = rise_rows[pl.ds(pl.multiple_of(me * share, share), share), :]
    row_part = jnp.concatenate([row_part[:, :grid], row_part], axis=1)
    col_part = jnp.concatenate([rise_cols[:grid], rise_cols[...]], axis=0)

    def include(bounds, values):
        high, low = high_low(jnp.concatenate(values, axis=1))
        wide = dot(row_part, jnp.concatenate([high, low, high], axis=0))
        wide = jnp.concatenate([wide[:, j * grid : (j + 1) * grid] for j in range(len(values))], axis=0)
        high, low = high_low(wide)
        blurred = dot(jnp.concatenate([high, low, high], axis=1), col_part)
        for j in range(len(values)):
            one = blurred[j * share : (j + 1) * share]
            bounds = (one, one) if bounds is None else (
                jnp.maximum(bounds[0], one),
                jnp.minimum(bounds[1], one),
            )
        return bounds

    def theirs(numbers):
        found = []
        for number in numbers:
            for step in range(1, n_cond):
                swap(number, step).wait_recv()
                found += [arrived[step - 1, c] for c in bunches[number]]
        return found

    early = theirs(range(len(bunches) - 2))
    bounds = include(None, [level[c] for c in range(conds)] + early)
    for i in ORDER:

        @pl.when(sends[i])
        def _():
            for q in targets(i):
                halo(i, q).wait_send()

    @pl.when(me == near)
    def _():
        for q in range(near):
            forward(q).wait_send()

    bounds = include(bounds, theirs(range(max(len(bunches) - 2, 0), len(bunches))))
    high_out[0] = bounds[0]
    low_out[0] = bounds[1]
    for step in range(1, n_cond):
        for number in range(len(bunches)):
            swap(number, step).wait_send()


def finish(high, low, high_out, low_out, staged):
    rows = high.shape[1] // WRITES

    def write(sem):
        copies = []
        for n in range(WRITES):
            piece = pl.ds(n * rows, rows)
            for which, (src, dst) in enumerate(((high, high_out), (low, low_out))):
                staged[which, piece] = jax.nn.sigmoid(src[0, piece])
                copies.append(
                    pltpu.make_async_copy(
                        staged.at[which, piece], dst.at[0, piece], sem.at[which, n]
                    )
                )
                copies[-1].start()
        for copy in copies:
            copy.wait()

    pl.run_scoped(write, pltpu.SemaphoreType.DMA((2, WRITES)))


def on_device(mask, kernels, socs_weight, dose, threshold):
    core = mask.shape[1]
    conds, kerns, band, _ = kernels.shape
    n_cond = lax.axis_size("cond")
    first_table, later_table, parts = make_tables(core, band)
    share = core // n_cond
    anywhere = pl.BlockSpec(memory_space=pl.ANY)
    vmem = pl.BlockSpec(memory_space=pltpu.VMEM)
    grid = 2 * band
    out = pltpu.VMEM((1, share, core), f32)

    def scoped(*refs):
        pl.run_scoped(
            functools.partial(body, parts, *refs),
            pltpu.SemaphoreType.DMA((8,)),
            pltpu.SemaphoreType.DMA((n_cond, 8)),
            pltpu.SemaphoreType.DMA((n_cond - 1, min(conds, 3))),
            pltpu.SemaphoreType.DMA((n_cond,)),
        )

    high, low = pl.pallas_call(
        scoped,
        out_shape=(out, out),
        in_specs=[anywhere] * 7,
        out_specs=(vmem, vmem),
        scratch_shapes=[
            pltpu.SMEM(socs_weight.shape, f32),
            pltpu.SMEM(dose.shape, f32),
            pltpu.SMEM(threshold.shape, f32),
            pltpu.VMEM((core, core), bf16),
            pltpu.VMEM(kernels.shape, bf16),
            pltpu.VMEM(first_table.shape, bf16),
            pltpu.VMEM(later_table.shape, bf16),
            pltpu.VMEM((2, 3, MARGIN, 2 * band), bf16),
            pltpu.VMEM((2, 3, MARGIN, 2 * band), bf16),
            pltpu.VMEM((2, band, 2 * MARGIN), bf16),
            pltpu.VMEM((2, band, 2 * MARGIN), bf16),
            pltpu.VMEM((conds, grid, grid), f32),
            pltpu.VMEM((n_cond - 1, conds, grid, grid), f32),
            pltpu.SemaphoreType.DMA((8,)),
            pltpu.SemaphoreType.DMA((n_cond - 1, min(conds, 3))),
            pltpu.SemaphoreType.DMA,
            pltpu.VMEM((2 * MARGIN, 2 * band), bf16),
            pltpu.VMEM((2, band, 2 * band), f32),
            pltpu.VMEM(kernels.shape, f32),
            pltpu.VMEM(kernels.shape, f32),
        ],
        compiler_params=pltpu.CompilerParams(collective_id=0, has_side_effects=True),
    )(mask, kernels, socs_weight, dose, threshold, jnp.asarray(first_table), jnp.asarray(later_table))
    out = jax.ShapeDtypeStruct((1, share, core), f32)
    return pl.pallas_call(
        finish,
        out_shape=(out, out),
        in_specs=[vmem] * 2,
        out_specs=(anywhere, anywhere),
        scratch_shapes=[pltpu.VMEM((2, share, core), f32)],
    )(*(pltpu.with_memory_space_constraint(x, pltpu.VMEM) for x in (high, low)))


def solution(mesh):
    return jax.shard_map(
        on_device,
        mesh=mesh,
        in_specs=(
            P(("parts", "tile"), None, None),
            P("cond", None, None, None),
            P("cond", None),
            P("cond"),
            P("cond"),
        ),
        out_specs=(P(("parts", "tile"), "cond", None), P(("parts", "tile"), "cond", None)),
        check_vma=False,
    )
```

```python
import functools

import jax
import jax.numpy as jnp
import ml_dtypes
import numpy as np
from jax import lax
from jax.experimental import pallas as pl
from jax.experimental.pallas import tpu as pltpu
from jax.sharding import PartitionSpec as P

MARGIN = 64
BLUR = 8
GROUP = 4
AHEAD = 3
DELAY = 2
PIECES = 8
WRITES = 8
SWAPS = 1
ORDER = (4, 3, 0, 1, 2, 7, 6, 5)

diffusion = 2.0
steepness = 8.0
bf16 = jnp.bfloat16
f32 = jnp.float32


def trig(turns, period):
    angle = 2.0 * np.pi * (turns % period) / period
    return np.cos(angle), np.sin(angle)


def split(table):
    high = table.astype(ml_dtypes.bfloat16)
    low = (table - high.astype(np.float64)).astype(ml_dtypes.bfloat16)
    return high, low


def make_tables(core, band):
    pad = core + 2 * MARGIN
    grid = 2 * band
    freq = np.arange(band) - band // 2
    cos_in, sin_in = trig(np.arange(pad)[:, None] * freq[None, :], pad)
    order = np.r_[MARGIN : MARGIN + core, 0:MARGIN, MARGIN + core : pad]
    row_table = np.concatenate([cos_in[order].T, -sin_in[order].T], axis=0)
    both = np.concatenate([cos_in, sin_in], axis=1)
    left, inner, right = both[:MARGIN], both[MARGIN : MARGIN + core], both[MARGIN + core :]
    gap = np.zeros((core - 2 * MARGIN, 2 * band))
    edges = np.concatenate([right, gap, left], axis=0)
    first_table = np.concatenate(
        [row_table[:, :core], np.concatenate([inner, edges], axis=1)], axis=0
    )
    strips = []
    for strip in (left, right):
        cos, sin = strip[:, :band], strip[:, band:]
        strips.append(np.concatenate([cos, cos, sin, -sin], axis=1))
        strips.append(np.concatenate([sin, sin, -cos, cos], axis=1))
    side_table = np.concatenate(strips, axis=0)
    cos_grid, sin_grid = trig(np.arange(grid)[:, None] * freq[None, :], grid)
    half_table = np.block([[cos_grid.T, sin_grid.T], [-sin_grid.T, cos_grid.T]])
    field_table = np.concatenate(
        [np.concatenate([cos_grid, -sin_grid], axis=1), np.concatenate([sin_grid, cos_grid], axis=1)], axis=1
    )
    pixel = np.arange(core + 2 * BLUR) + MARGIN - BLUR
    phase = pixel[:, None] / pad - np.arange(grid)[None, :] / grid
    waves = np.arange(1, band)
    interp = (1.0 + 2.0 * np.cos(2.0 * np.pi * phase[:, :, None] * waves).sum(-1)) / grid
    offset = np.arange(core + 2 * BLUR)[None, :] - np.arange(core)[:, None] - BLUR
    taps = np.exp(-(offset**2) / (2.0 * diffusion**2)) * (np.abs(offset) <= BLUR)
    reach = np.arange(-BLUR, BLUR + 1)
    taps = taps / np.exp(-(reach**2) / (2.0 * diffusion**2)).sum()
    rise = taps @ interp
    high, low = split(rise)
    rise_rows = np.concatenate([high, low], axis=1)
    rise_cols = np.concatenate([high.T, low.T], axis=0)
    outer_rows = np.concatenate([row_table[:, core:], np.zeros((2 * band, 2 * band))], axis=1)
    later = (side_table, half_table, field_table, outer_rows, rise_cols, rise_rows)
    bounds = np.cumsum([0] + [len(t) for t in later])
    later = np.concatenate([t.astype(ml_dtypes.bfloat16) for t in later], axis=0)
    return first_table.astype(ml_dtypes.bfloat16), later, [int(n) for n in bounds]


def neighbours():
    count = lax.axis_size("tile")
    columns = min(8, count // 2)
    rows = count // columns
    me = lax.axis_index("tile")
    position = lax.rem(me + columns // 2, count)
    column = lax.rem(position, columns)
    row = lax.div(position, columns)
    found = []
    for down in (-1, 0, 1):
        for right in (-1, 0, 1):
            if down == 0 and right == 0:
                continue
            flag = (row + down >= 0) & (row + down < rows)
            flag = flag & (column + right >= 0) & (column + right < columns)
            there = lax.rem(me + down * columns + right + count, count)
            found.append((down, right, flag, there))
    return found


def slot(down, right):
    return (0 if down < 0 else 1, right % 3) if down else (0 if right < 0 else 1,)


def high_low(value):
    high = value.astype(bf16)
    return high, (value - high.astype(f32)).astype(bf16)


def dot(a, b):
    return jnp.dot(a, b, preferred_element_type=f32)


def start_split(load):
    src, dst, sem = load
    rows = dst.shape[0] // PIECES
    for n in range(PIECES):
        piece = pl.ds(n * rows, rows)
        pltpu.make_async_copy(src.at[piece], dst.at[piece], sem).start()


def body(
    parts,
    mask_hbm,
    kern_hbm,
    weight_hbm,
    dose_hbm,
    threshold_hbm,
    first_hbm,
    later_hbm,
    high_out,
    low_out,
    weight,
    dose,
    threshold,
    tile,
    kern,
    first_table,
    later_table,
    rows_out,
    rows_in,
    side_out,
    side_in,
    level,
    arrived,
    halo_recv,
    swap_recv,
    forward_recv,
    outer,
    spec,
    plain,
    turned,
    load_sem,
    halo_send,
    swap_send,
    forward_send,
):
    core = mask_hbm.shape[1]
    conds, kerns, band, _ = kern_hbm.shape
    grid = 2 * band
    side_table, half_table, field_table, outer_rows, rise_cols, rise_rows = (
        later_table.at[pl.ds(lo, hi - lo)] for lo, hi in zip(parts[:-1], parts[1:])
    )
    row_table = first_table.at[pl.ds(0, grid)]
    inner_table = first_table.at[pl.ds(grid, core), pl.ds(0, grid)]
    edge_table = first_table.at[pl.ds(grid, core), pl.ds(grid, grid)]

    loads = [
        (src, dst, load_sem.at[i])
        for i, (src, dst) in enumerate(
            (
                (mask_hbm.at[0], tile),
                (first_hbm.at[pl.ds(0, grid)], first_table.at[pl.ds(0, grid)]),
                (first_hbm.at[pl.ds(grid, core)], first_table.at[pl.ds(grid, core)]),
                (kern_hbm, kern),
                (weight_hbm, weight),
                (dose_hbm, dose),
                (threshold_hbm, threshold),
                (later_hbm, later_table),
            )
        )
    ]
    for load in loads[:2]:
        start_split(load)

    middle_of = core // 2
    n_cond = lax.axis_size("cond")
    me = lax.axis_index("cond")
    near = n_cond - 1
    around = neighbours()
    tiles = lax.axis_size("tile")
    sends = [flag & jnp.where(there <= tiles // 2 + 1, me == near, me == 0) for _, _, flag, there in around]

    def targets(i):
        return (near,) if around[i][0] else tuple(range(n_cond))

    caller = jnp.where(lax.axis_index("tile") <= tiles // 2 + 1, near, 0)
    barrier = pltpu.get_barrier_semaphore()
    for i in reversed(range(len(around))):
        down, _, flag, there = around[i]

        @pl.when(flag & (me == near) if down else flag)
        def _():
            pl.semaphore_signal(barrier, inc=1, device_id={"tile": there, "cond": caller})

    for step in range(1, n_cond):
        pl.semaphore_signal(barrier, inc=1, device_id={"cond": lax.rem(me + step, n_cond)})
    start_split(loads[2])
    for down, right, flag, _ in around:

        @pl.when(jnp.logical_not(flag))
        def _():
            buffer = rows_in if down else side_in
            at = slot(down, right)
            buffer[at] = jnp.zeros(buffer.shape[len(at) :], bf16)

    for load in loads[:2]:
        pltpu.make_async_copy(*load).wait()
    for load in loads[3:]:
        pltpu.make_async_copy(*load).start()
    lane = lax.broadcasted_iota(jnp.int32, (band, 2 * band), 1)
    first = lane < band
    wide_first = lax.broadcasted_iota(jnp.int32, (core, grid), 1) < band
    edges = jnp.where(wide_first, tile[:, :grid], tile[:, core - grid :])
    edges = dot(row_table[...], edges)
    turned_edges = pltpu.roll(edges, band, 1)
    side_out[0] = jnp.where(first, edges[:band], turned_edges[band:]).astype(bf16)
    side_out[1] = jnp.where(first, turned_edges[:band], edges[band:]).astype(bf16)
    peers = n_cond - 1
    for i, send in enumerate(sends):
        peers = peers + jnp.where(send, len(targets(i)), 0)
    pl.semaphore_wait(barrier, peers)

    def halo(i, q):
        down, right, _, there = around[i]
        outgoing, incoming = (rows_out, rows_in) if down else (side_out, side_in)
        return pltpu.make_async_remote_copy(
            src_ref=outgoing.at[slot(down, right)],
            dst_ref=incoming.at[slot(-down, -right)],
            send_sem=halo_send.at[q, i],
            recv_sem=halo_recv.at[len(around) - 1 - i],
            device_id={"tile": there, "cond": q},
        )

    def depart(numbers):
        for i in numbers:

            @pl.when(sends[i])
            def _():
                for q in targets(i):
                    halo(i, q).start()

    depart(i for i in ORDER if not around[i][0])
    pltpu.make_async_copy(*loads[2]).wait()
    strips = jnp.concatenate([tile[:MARGIN, :], tile[core - MARGIN :, :]], axis=0)
    blocks = [
        dot(strips, inner_table[...]).astype(bf16),
        dot(strips[:, middle_of:], edge_table[middle_of:, :]).astype(bf16),
        dot(strips[:, :middle_of], edge_table[:middle_of, :]).astype(bf16),
    ]
    for at in range(2):
        for lanes in range(3):
            rows_out[at, lanes] = blocks[lanes][at * MARGIN : (at + 1) * MARGIN]
    depart(i for i in ORDER if around[i][0])

    for load in loads[3:]:
        pltpu.make_async_copy(*load).wait()
    middle = dot(row_table[...], tile[...]).astype(bf16)
    inner = dot(middle, inner_table[...])
    tops = []
    for c in range(conds):
        weight_sum = weight[c, 0]
        for k in range(1, kerns):
            weight_sum = weight_sum + weight[c, k]
        gain = jnp.full((8, grid), steepness * dose[c], f32) / jnp.full((8, grid), weight_sum, f32)
        tops.append(steepness * threshold[c])
        for k in range(kerns):
            root = jnp.sqrt(gain * weight[c, k]) * (1.0 / ((core + 2 * MARGIN) * band))
            scaled = kern[c, k].astype(f32) * root[0:1]
            plain[c, k] = scaled
            turned[c, k] = pltpu.roll(scaled, band, 1)

    def arrive(numbers):
        for i in numbers:

            @pl.when(around[i][2])
            def _():
                halo(len(around) - 1 - i, 0).wait_recv()

    def forward(q):
        return pltpu.make_async_remote_copy(
            src_ref=outer,
            dst_ref=outer,
            send_sem=forward_send.at[q],
            recv_sem=forward_recv,
            device_id={"cond": q},
        )

    def from_rows():
        quarters = inner + dot(outer_rows[:, : 2 * MARGIN], outer[...])
        turned_quarters = pltpu.roll(quarters, band, 1)
        top, bottom = quarters[:band], quarters[band:]
        top_turned, bottom_turned = turned_quarters[:band], turned_quarters[band:]
        same = jnp.where(first, top + bottom_turned, top_turned + bottom)
        cross = jnp.where(first, top_turned - bottom, bottom_turned - top)
        return same, cross

    def from_sides(same, cross):
        sides = dot(jnp.concatenate([side_in[0], side_in[1]], axis=1), side_table[...])
        spec[0] = same + sides[:, : 2 * band]
        spec[1] = cross + sides[:, 2 * band :]

    def departed():
        for i in ORDER:

            @pl.when(sends[i])
            def _():
                for q in targets(i):
                    halo(i, q).wait_send()

    beside = [i for i in range(len(around)) if not around[i][0]]

    @pl.when(me == near)
    def _():
        arrive(i for i in range(len(around)) if around[i][0])
        rows = rows_in[...].astype(f32)
        rows = rows[:, 0] + rows[:, 1] + rows[:, 2]
        outer[...] = rows.reshape(2 * MARGIN, 2 * band).astype(bf16)
        for q in range(near):
            forward(q).start()
        same, cross = from_rows()
        arrive(beside)
        from_sides(same, cross)

    @pl.when(me != near)
    def _():
        arrive(beside)
        departed()
        forward(0).wait_recv()
        from_sides(*from_rows())

    spec_same, spec_cross = spec[0], spec[1]

    bunches = [list(range(max(conds - 2, 0)))] + [[c] for c in range(max(conds - 2, 0), conds)]
    bunches = [bunch for bunch in bunches if bunch]

    def swap(i, step, rows=pl.ds(0, grid)):
        chosen = pl.ds(bunches[i][0], len(bunches[i]))
        return pltpu.make_async_remote_copy(
            src_ref=level.at[chosen, rows],
            dst_ref=arrived.at[step - 1, chosen, rows],
            send_sem=swap_send.at[step - 1, i],
            recv_sem=swap_recv.at[step - 1, i],
            device_id={"cond": lax.rem(me + step, n_cond)},
        )

    def halves(c, start, size):
        prod = [
            (spec_same * plain[c, k] + spec_cross * turned[c, k]).astype(bf16)
            for k in range(start, start + size)
        ]
        half = dot(jnp.concatenate(prod, axis=0), half_table[...]).astype(bf16)
        return [half[j * band : (j + 1) * band] for j in range(size)]

    def powers(total, pair):
        stacked = jnp.concatenate(
            [
                jnp.concatenate([h[:, :grid] for h in pair], axis=1),
                jnp.concatenate([h[:, grid:] for h in pair], axis=1),
            ],
            axis=0,
        )
        sampling = jnp.concatenate([field_table[:, :grid], field_table[:, grid:]], axis=0)
        field = dot(sampling, stacked)
        power = field[:grid] * field[:grid] + field[grid:] * field[grid:]
        for j in range(len(pair)):
            total = total + power[:, j * grid : (j + 1) * grid]
        return total

    groups = [
        (c, start, min(GROUP, kerns - start)) for c in range(conds) for start in range(0, kerns, GROUP)
    ]
    ready = [halves(*groups[i]) for i in range(min(AHEAD, len(groups)))]
    total = None
    due = []
    for i, (c, start, size) in enumerate(groups):
        if i + AHEAD < len(groups):
            ready.append(halves(*groups[i + AHEAD]))
        if start == 0:
            total = jnp.full((grid, grid), -tops[c], f32)
        half = ready[i]
        for j in range(0, size, 2):
            total = powers(total, half[j : j + 2])
        if start + size == kerns:
            level[c] = total
            for number, bunch in enumerate(bunches):
                if c == bunch[-1]:
                    due.append((i + DELAY, number))
        while due and (due[0][0] <= i or i + 1 == len(groups)):
            number = due.pop(0)[1]
            for step in range(1, n_cond):
                for n in range(SWAPS):
                    swap(number, step, pl.ds(n * (grid // SWAPS), grid // SWAPS)).start()

    share = high_out.shape[1]
    row_part = rise_rows[pl.ds(pl.multiple_of(me * share, share), share), :]
    row_part = jnp.concatenate([row_part, row_part[:, :grid]], axis=1)
    col_part = jnp.concatenate([rise_cols[...], rise_cols[:grid]], axis=0)

    def include(bounds, values):
        high, low = high_low(jnp.concatenate(values, axis=1))
        wide = dot(row_part, jnp.concatenate([high, high, low], axis=0))
        half = (len(values) + 1) // 2
        for some in (range(half), range(half, len(values))):
            if not len(some):
                continue
            part = jnp.concatenate([wide[:, j * grid : (j + 1) * grid] for j in some], axis=0)
            high, low = high_low(part)
            blurred = dot(jnp.concatenate([high, high, low], axis=1), col_part)
            for j in range(len(some)):
                one = blurred[j * share : (j + 1) * share]
                bounds = (one, one) if bounds is None else (
                    jnp.maximum(bounds[0], one),
                    jnp.minimum(bounds[1], one),
                )
        return bounds

    def theirs(numbers):
        found = []
        for number in numbers:
            for step in range(1, n_cond):
                swap(number, step).wait_recv()
                found += [arrived[step - 1, c] for c in bunches[number]]
        return found

    early = theirs(range(len(bunches) - 2))
    bounds = include(None, [level[c] for c in range(conds)] + early)
    @pl.when(me == near)
    def _():
        departed()
        for q in range(near):
            forward(q).wait_send()

    bounds = include(bounds, theirs(range(max(len(bunches) - 2, 0), len(bunches))))
    high_out[0] = bounds[0]
    low_out[0] = bounds[1]
    for step in range(1, n_cond):
        for number in range(len(bunches)):
            swap(number, step).wait_send()


def finish(high, low, high_out, low_out, staged):
    rows = high.shape[1] // WRITES

    def write(sem):
        copies = []
        for n in range(WRITES):
            piece = pl.ds(n * rows, rows)
            for which, (src, dst) in enumerate(((high, high_out), (low, low_out))):
                staged[which, piece] = jax.nn.sigmoid(src[0, piece])
                copies.append(
                    pltpu.make_async_copy(
                        staged.at[which, piece], dst.at[0, piece], sem.at[which, n]
                    )
                )
                copies[-1].start()
        for copy in copies:
            copy.wait()

    pl.run_scoped(write, pltpu.SemaphoreType.DMA((2, WRITES)))


def on_device(mask, kernels, socs_weight, dose, threshold):
    core = mask.shape[1]
    conds, kerns, band, _ = kernels.shape
    n_cond = lax.axis_size("cond")
    first_table, later_table, parts = make_tables(core, band)
    share = core // n_cond
    anywhere = pl.BlockSpec(memory_space=pl.ANY)
    vmem = pl.BlockSpec(memory_space=pltpu.VMEM)
    grid = 2 * band
    out = pltpu.VMEM((1, share, core), f32)

    def scoped(*refs):
        pl.run_scoped(
            functools.partial(body, parts, *refs),
            pltpu.SemaphoreType.DMA((8,)),
            pltpu.SemaphoreType.DMA((n_cond, 8)),
            pltpu.SemaphoreType.DMA((n_cond - 1, min(conds, 3))),
            pltpu.SemaphoreType.DMA((n_cond,)),
        )

    high, low = pl.pallas_call(
        scoped,
        out_shape=(out, out),
        in_specs=[anywhere] * 7,
        out_specs=(vmem, vmem),
        scratch_shapes=[
            pltpu.SMEM(socs_weight.shape, f32),
            pltpu.SMEM(dose.shape, f32),
            pltpu.SMEM(threshold.shape, f32),
            pltpu.VMEM((core, core), bf16),
            pltpu.VMEM(kernels.shape, bf16),
            pltpu.VMEM(first_table.shape, bf16),
            pltpu.VMEM(later_table.shape, bf16),
            pltpu.VMEM((2, 3, MARGIN, 2 * band), bf16),
            pltpu.VMEM((2, 3, MARGIN, 2 * band), bf16),
            pltpu.VMEM((2, band, 2 * MARGIN), bf16),
            pltpu.VMEM((2, band, 2 * MARGIN), bf16),
            pltpu.VMEM((conds, grid, grid), f32),
            pltpu.VMEM((n_cond - 1, conds, grid, grid), f32),
            pltpu.SemaphoreType.DMA((8,)),
            pltpu.SemaphoreType.DMA((n_cond - 1, min(conds, 3))),
            pltpu.SemaphoreType.DMA,
            pltpu.VMEM((2 * MARGIN, 2 * band), bf16),
            pltpu.VMEM((2, band, 2 * band), f32),
            pltpu.VMEM(kernels.shape, f32),
            pltpu.VMEM(kernels.shape, f32),
        ],
        compiler_params=pltpu.CompilerParams(collective_id=0, has_side_effects=True),
    )(mask, kernels, socs_weight, dose, threshold, jnp.asarray(first_table), jnp.asarray(later_table))
    out = jax.ShapeDtypeStruct((1, share, core), f32)
    return pl.pallas_call(
        finish,
        out_shape=(out, out),
        in_specs=[vmem] * 2,
        out_specs=(anywhere, anywhere),
        scratch_shapes=[pltpu.VMEM((2, share, core), f32)],
    )(*(pltpu.with_memory_space_constraint(x, pltpu.VMEM) for x in (high, low)))


def solution(mesh):
    return jax.shard_map(
        on_device,
        mesh=mesh,
        in_specs=(
            P(("parts", "tile"), None, None),
            P("cond", None, None, None),
            P("cond", None),
            P("cond"),
            P("cond"),
        ),
        out_specs=(P(("parts", "tile"), "cond", None), P(("parts", "tile"), "cond", None)),
        check_vma=False,
    )
```

```python
import functools

import jax
import jax.numpy as jnp
import ml_dtypes
import numpy as np
from jax import lax
from jax.experimental import pallas as pl
from jax.experimental.pallas import tpu as pltpu
from jax.sharding import PartitionSpec as P

MARGIN = 64
BLUR = 8
GROUP = 4
AHEAD = 3
DELAY = 2
PIECES = 8
WRITES = 8
SWAPS = 1
ORDER = (4, 3, 0, 1, 2, 7, 6, 5)

diffusion = 2.0
steepness = 8.0
bf16 = jnp.bfloat16
f32 = jnp.float32


def trig(turns, period):
    angle = 2.0 * np.pi * (turns % period) / period
    return np.cos(angle), np.sin(angle)


def split(table):
    high = table.astype(ml_dtypes.bfloat16)
    low = (table - high.astype(np.float64)).astype(ml_dtypes.bfloat16)
    return high, low


def make_tables(core, band):
    pad = core + 2 * MARGIN
    grid = 2 * band
    freq = np.arange(band) - band // 2
    cos_in, sin_in = trig(np.arange(pad)[:, None] * freq[None, :], pad)
    order = np.r_[MARGIN : MARGIN + core, 0:MARGIN, MARGIN + core : pad]
    row_table = np.concatenate([cos_in[order].T, -sin_in[order].T], axis=0)
    both = np.concatenate([cos_in, sin_in], axis=1)
    left, inner, right = both[:MARGIN], both[MARGIN : MARGIN + core], both[MARGIN + core :]
    gap = np.zeros((core - 2 * MARGIN, 2 * band))
    edges = np.concatenate([right, gap, left], axis=0)
    first_table = np.concatenate(
        [row_table[:, :core], np.concatenate([inner, edges], axis=1)], axis=0
    )
    strips = []
    for strip in (left, right):
        cos, sin = strip[:, :band], strip[:, band:]
        strips.append(np.concatenate([cos, cos, sin, -sin], axis=1))
        strips.append(np.concatenate([sin, sin, -cos, cos], axis=1))
    side_table = np.concatenate(strips, axis=0)
    cos_grid, sin_grid = trig(np.arange(grid)[:, None] * freq[None, :], grid)
    half_table = np.block([[cos_grid.T, sin_grid.T], [-sin_grid.T, cos_grid.T]])
    field_table = np.concatenate(
        [np.concatenate([cos_grid, -sin_grid], axis=1), np.concatenate([sin_grid, cos_grid], axis=1)], axis=1
    )
    pixel = np.arange(core + 2 * BLUR) + MARGIN - BLUR
    phase = pixel[:, None] / pad - np.arange(grid)[None, :] / grid
    waves = np.arange(1, band)
    interp = (1.0 + 2.0 * np.cos(2.0 * np.pi * phase[:, :, None] * waves).sum(-1)) / grid
    offset = np.arange(core + 2 * BLUR)[None, :] - np.arange(core)[:, None] - BLUR
    taps = np.exp(-(offset**2) / (2.0 * diffusion**2)) * (np.abs(offset) <= BLUR)
    reach = np.arange(-BLUR, BLUR + 1)
    taps = taps / np.exp(-(reach**2) / (2.0 * diffusion**2)).sum()
    rise = taps @ interp
    high, low = split(rise)
    rise_rows = np.concatenate([high, low], axis=1)
    rise_cols = np.concatenate([high.T, low.T], axis=0)
    outer_rows = np.concatenate([row_table[:, core:], np.zeros((2 * band, 2 * band))], axis=1)
    later = (side_table, half_table, field_table, outer_rows, rise_cols, rise_rows)
    bounds = np.cumsum([0] + [len(t) for t in later])
    later = np.concatenate([t.astype(ml_dtypes.bfloat16) for t in later], axis=0)
    return first_table.astype(ml_dtypes.bfloat16), later, [int(n) for n in bounds]


def neighbours():
    count = lax.axis_size("tile")
    columns = min(8, count // 2)
    rows = count // columns
    me = lax.axis_index("tile")
    position = lax.rem(me + columns // 2, count)
    column = lax.rem(position, columns)
    row = lax.div(position, columns)
    found = []
    for down in (-1, 0, 1):
        for right in (-1, 0, 1):
            if down == 0 and right == 0:
                continue
            flag = (row + down >= 0) & (row + down < rows)
            flag = flag & (column + right >= 0) & (column + right < columns)
            there = lax.rem(me + down * columns + right + count, count)
            found.append((down, right, flag, there))
    return found


def slot(down, right):
    return (0 if down < 0 else 1, right % 3) if down else (0 if right < 0 else 1,)


def high_low(value):
    high = value.astype(bf16)
    return high, (value - high.astype(f32)).astype(bf16)


def dot(a, b):
    return jnp.dot(a, b, preferred_element_type=f32)


def start_split(load):
    src, dst, sem = load
    rows = dst.shape[0] // PIECES
    for n in range(PIECES):
        piece = pl.ds(n * rows, rows)
        pltpu.make_async_copy(src.at[piece], dst.at[piece], sem).start()


def body(
    parts,
    mask_hbm,
    kern_hbm,
    weight_hbm,
    dose_hbm,
    threshold_hbm,
    first_hbm,
    later_hbm,
    high_out,
    low_out,
    weight,
    dose,
    threshold,
    tile,
    kern,
    first_table,
    later_table,
    rows_out,
    rows_in,
    side_out,
    side_in,
    level,
    arrived,
    halo_recv,
    swap_recv,
    forward_recv,
    outer,
    spec,
    plain,
    turned,
    load_sem,
    halo_send,
    swap_send,
    forward_send,
):
    core = mask_hbm.shape[1]
    conds, kerns, band, _ = kern_hbm.shape
    grid = 2 * band
    side_table, half_table, field_table, outer_rows, rise_cols, rise_rows = (
        later_table.at[pl.ds(lo, hi - lo)] for lo, hi in zip(parts[:-1], parts[1:])
    )
    row_table = first_table.at[pl.ds(0, grid)]
    inner_table = first_table.at[pl.ds(grid, core), pl.ds(0, grid)]
    edge_table = first_table.at[pl.ds(grid, core), pl.ds(grid, grid)]

    loads = [
        (src, dst, load_sem.at[i])
        for i, (src, dst) in enumerate(
            (
                (mask_hbm.at[0], tile),
                (first_hbm.at[pl.ds(0, grid)], first_table.at[pl.ds(0, grid)]),
                (first_hbm.at[pl.ds(grid, core)], first_table.at[pl.ds(grid, core)]),
                (kern_hbm, kern),
                (weight_hbm, weight),
                (dose_hbm, dose),
                (threshold_hbm, threshold),
                (later_hbm, later_table),
            )
        )
    ]
    for load in loads[:2]:
        start_split(load)

    middle_of = core // 2
    n_cond = lax.axis_size("cond")
    me = lax.axis_index("cond")
    near = n_cond - 1
    around = neighbours()
    tiles = lax.axis_size("tile")
    sends = [flag & jnp.where(there <= tiles // 2 + 1, me == near, me == 0) for _, _, flag, there in around]

    def targets(i):
        return (near,) if around[i][0] else tuple(range(n_cond))

    caller = jnp.where(lax.axis_index("tile") <= tiles // 2 + 1, near, 0)
    barrier = pltpu.get_barrier_semaphore()
    for i in reversed(range(len(around))):
        down, _, flag, there = around[i]

        @pl.when(flag & (me == near) if down else flag)
        def _():
            pl.semaphore_signal(barrier, inc=1, device_id={"tile": there, "cond": caller})

    for step in range(1, n_cond):
        pl.semaphore_signal(barrier, inc=1, device_id={"cond": lax.rem(me + step, n_cond)})
    start_split(loads[2])
    for down, right, flag, _ in around:

        @pl.when(jnp.logical_not(flag))
        def _():
            buffer = rows_in if down else side_in
            at = slot(down, right)
            buffer[at] = jnp.zeros(buffer.shape[len(at) :], bf16)

    for load in loads[:2]:
        pltpu.make_async_copy(*load).wait()
    for load in loads[3:]:
        pltpu.make_async_copy(*load).start()
    lane = lax.broadcasted_iota(jnp.int32, (band, 2 * band), 1)
    first = lane < band
    wide_first = lax.broadcasted_iota(jnp.int32, (core, grid), 1) < band
    edges = jnp.where(wide_first, tile[:, :grid], tile[:, core - grid :])
    edges = dot(row_table[...], edges)
    turned_edges = pltpu.roll(edges, band, 1)
    side_out[0] = jnp.where(first, edges[:band], turned_edges[band:]).astype(bf16)
    side_out[1] = jnp.where(first, turned_edges[:band], edges[band:]).astype(bf16)
    peers = n_cond - 1
    for i, send in enumerate(sends):
        peers = peers + jnp.where(send, len(targets(i)), 0)
    pl.semaphore_wait(barrier, peers)

    def halo(i, q):
        down, right, _, there = around[i]
        outgoing, incoming = (rows_out, rows_in) if down else (side_out, side_in)
        return pltpu.make_async_remote_copy(
            src_ref=outgoing.at[slot(down, right)],
            dst_ref=incoming.at[slot(-down, -right)],
            send_sem=halo_send.at[q, i],
            recv_sem=halo_recv.at[len(around) - 1 - i],
            device_id={"tile": there, "cond": q},
        )

    def depart(numbers):
        for i in numbers:

            @pl.when(sends[i])
            def _():
                for q in targets(i):
                    halo(i, q).start()

    depart(i for i in ORDER if not around[i][0])
    pltpu.make_async_copy(*loads[2]).wait()
    strips = jnp.concatenate([tile[:MARGIN, :], tile[core - MARGIN :, :]], axis=0)
    blocks = [
        dot(strips, inner_table[...]).astype(bf16),
        dot(strips[:, middle_of:], edge_table[middle_of:, :]).astype(bf16),
        dot(strips[:, :middle_of], edge_table[:middle_of, :]).astype(bf16),
    ]
    for at in range(2):
        for lanes in range(3):
            rows_out[at, lanes] = blocks[lanes][at * MARGIN : (at + 1) * MARGIN]
    depart(i for i in ORDER if around[i][0])

    for load in loads[3:]:
        pltpu.make_async_copy(*load).wait()
    middle = dot(row_table[...], tile[...]).astype(bf16)
    inner = dot(middle, inner_table[...])
    tops = []
    for c in range(conds):
        weight_sum = weight[c, 0]
        for k in range(1, kerns):
            weight_sum = weight_sum + weight[c, k]
        gain = jnp.full((8, grid), steepness * dose[c], f32) / jnp.full((8, grid), weight_sum, f32)
        tops.append(steepness * threshold[c])
        for k in range(kerns):
            root = jnp.sqrt(gain * weight[c, k]) * (1.0 / ((core + 2 * MARGIN) * band))
            scaled = kern[c, k].astype(f32) * root[0:1]
            plain[c, k] = scaled
            turned[c, k] = pltpu.roll(scaled, band, 1)

    def arrive(numbers):
        for i in numbers:

            @pl.when(around[i][2])
            def _():
                halo(len(around) - 1 - i, 0).wait_recv()

    def forward(q):
        return pltpu.make_async_remote_copy(
            src_ref=outer,
            dst_ref=outer,
            send_sem=forward_send.at[q],
            recv_sem=forward_recv,
            device_id={"cond": q},
        )

    def from_rows():
        quarters = inner + dot(outer_rows[:, : 2 * MARGIN], outer[...])
        turned_quarters = pltpu.roll(quarters, band, 1)
        top, bottom = quarters[:band], quarters[band:]
        top_turned, bottom_turned = turned_quarters[:band], turned_quarters[band:]
        same = jnp.where(first, top + bottom_turned, top_turned + bottom)
        cross = jnp.where(first, top_turned - bottom, bottom_turned - top)
        return same, cross

    def from_sides(same, cross):
        sides = dot(jnp.concatenate([side_in[0], side_in[1]], axis=1), side_table[...])
        spec[0] = same + sides[:, : 2 * band]
        spec[1] = cross + sides[:, 2 * band :]

    def departed():
        for i in ORDER:

            @pl.when(sends[i])
            def _():
                for q in targets(i):
                    halo(i, q).wait_send()

    beside = [i for i in range(len(around)) if not around[i][0]]

    @pl.when(me == near)
    def _():
        arrive(i for i in range(len(around)) if around[i][0])
        rows = rows_in[...].astype(f32)
        rows = rows[:, 0] + rows[:, 1] + rows[:, 2]
        outer[...] = rows.reshape(2 * MARGIN, 2 * band).astype(bf16)
        for q in range(near):
            forward(q).start()
        same, cross = from_rows()
        arrive(beside)
        from_sides(same, cross)

    @pl.when(me != near)
    def _():
        arrive(beside)
        departed()
        forward(0).wait_recv()
        from_sides(*from_rows())

    spec_same, spec_cross = spec[0], spec[1]

    bunches = [list(range(max(conds - 2, 0)))] + [[c] for c in range(max(conds - 2, 0), conds)]
    bunches = [bunch for bunch in bunches if bunch]

    def swap(i, step, rows=pl.ds(0, grid)):
        chosen = pl.ds(bunches[i][0], len(bunches[i]))
        return pltpu.make_async_remote_copy(
            src_ref=level.at[chosen, rows],
            dst_ref=arrived.at[step - 1, chosen, rows],
            send_sem=swap_send.at[step - 1, i],
            recv_sem=swap_recv.at[step - 1, i],
            device_id={"cond": lax.rem(me + step, n_cond)},
        )

    def halves(c, start, size):
        prod = [
            (spec_same * plain[c, k] + spec_cross * turned[c, k]).astype(bf16)
            for k in range(start, start + size)
        ]
        half = dot(jnp.concatenate(prod, axis=0), half_table[...]).astype(bf16)
        return [half[j * band : (j + 1) * band] for j in range(size)]

    def powers(total, pair):
        stacked = jnp.concatenate(
            [
                jnp.concatenate([h[:, :grid] for h in pair], axis=1),
                jnp.concatenate([h[:, grid:] for h in pair], axis=1),
            ],
            axis=0,
        )
        sampling = jnp.concatenate([field_table[:, :grid], field_table[:, grid:]], axis=0)
        field = dot(sampling, stacked)
        power = field[:grid] * field[:grid] + field[grid:] * field[grid:]
        for j in range(len(pair)):
            total = total + power[:, j * grid : (j + 1) * grid]
        return total

    groups = [
        (c, start, min(GROUP, kerns - start)) for c in range(conds) for start in range(0, kerns, GROUP)
    ]
    ready = [halves(*groups[i]) for i in range(min(AHEAD, len(groups)))]
    total = None
    due = []
    for i, (c, start, size) in enumerate(groups):
        if i + AHEAD < len(groups):
            ready.append(halves(*groups[i + AHEAD]))
        if start == 0:
            total = jnp.full((grid, grid), -tops[c], f32)
        half = ready[i]
        for j in range(0, size, 2):
            total = powers(total, half[j : j + 2])
        if start + size == kerns:
            level[c] = total
            for number, bunch in enumerate(bunches):
                if c == bunch[-1]:
                    due.append((i + DELAY, number))
        while due and (due[0][0] <= i or i + 1 == len(groups)):
            number = due.pop(0)[1]
            for step in range(1, n_cond):
                for n in range(SWAPS):
                    swap(number, step, pl.ds(n * (grid // SWAPS), grid // SWAPS)).start()

    share = high_out.shape[1]
    row_part = rise_rows[pl.ds(pl.multiple_of(me * share, share), share), :]
    row_part = jnp.concatenate([row_part, row_part[:, :grid]], axis=1)
    col_part = jnp.concatenate([rise_cols[...], rise_cols[:grid]], axis=0)

    def include(bounds, values):
        high, low = high_low(jnp.concatenate(values, axis=1))
        wide = dot(row_part, jnp.concatenate([high, high, low], axis=0))
        half = (len(values) + 1) // 2
        for some in (range(half), range(half, len(values))):
            if not len(some):
                continue
            part = jnp.concatenate([wide[:, j * grid : (j + 1) * grid] for j in some], axis=0)
            high, low = high_low(part)
            part = jnp.concatenate([high, high, low], axis=1)
            cut = len(part) if len(values) > 1 else len(part) // 2
            blurred = jnp.concatenate(
                [dot(part[n : n + cut], col_part) for n in range(0, len(part), cut)], axis=0
            )
            for j in range(len(some)):
                one = blurred[j * share : (j + 1) * share]
                bounds = (one, one) if bounds is None else (
                    jnp.maximum(bounds[0], one),
                    jnp.minimum(bounds[1], one),
                )
        return bounds

    def theirs(numbers):
        found = []
        for number in numbers:
            for step in range(1, n_cond):
                swap(number, step).wait_recv()
                found += [arrived[step - 1, c] for c in bunches[number]]
        return found

    early = theirs(range(len(bunches) - 2))
    bounds = include(None, [level[c] for c in range(conds)] + early)
    late_bunches = list(range(max(len(bunches) - 2, 0), len(bunches)))

    def conclude(rounds):
        result = bounds
        for numbers in rounds:
            result = include(result, theirs(numbers))
        high_out[0] = result[0]
        low_out[0] = result[1]

    @pl.when(me == near)
    def _():
        departed()
        for q in range(near):
            forward(q).wait_send()
        conclude([[number] for number in late_bunches])

    @pl.when(me != near)
    def _():
        conclude([late_bunches])

    for step in range(1, n_cond):
        for number in range(len(bunches)):
            swap(number, step).wait_send()


def finish(high, low, high_out, low_out, staged):
    rows = high.shape[1] // WRITES

    def write(sem):
        copies = []
        for n in range(WRITES):
            piece = pl.ds(n * rows, rows)
            for which, (src, dst) in enumerate(((high, high_out), (low, low_out))):
                staged[which, piece] = jax.nn.sigmoid(src[0, piece])
                copies.append(
                    pltpu.make_async_copy(
                        staged.at[which, piece], dst.at[0, piece], sem.at[which, n]
                    )
                )
                copies[-1].start()
        for copy in copies:
            copy.wait()

    pl.run_scoped(write, pltpu.SemaphoreType.DMA((2, WRITES)))


def on_device(mask, kernels, socs_weight, dose, threshold):
    core = mask.shape[1]
    conds, kerns, band, _ = kernels.shape
    n_cond = lax.axis_size("cond")
    first_table, later_table, parts = make_tables(core, band)
    share = core // n_cond
    anywhere = pl.BlockSpec(memory_space=pl.ANY)
    vmem = pl.BlockSpec(memory_space=pltpu.VMEM)
    grid = 2 * band
    out = pltpu.VMEM((1, share, core), f32)

    def scoped(*refs):
        pl.run_scoped(
            functools.partial(body, parts, *refs),
            pltpu.SemaphoreType.DMA((8,)),
            pltpu.SemaphoreType.DMA((n_cond, 8)),
            pltpu.SemaphoreType.DMA((n_cond - 1, min(conds, 3))),
            pltpu.SemaphoreType.DMA((n_cond,)),
        )

    high, low = pl.pallas_call(
        scoped,
        out_shape=(out, out),
        in_specs=[anywhere] * 7,
        out_specs=(vmem, vmem),
        scratch_shapes=[
            pltpu.SMEM(socs_weight.shape, f32),
            pltpu.SMEM(dose.shape, f32),
            pltpu.SMEM(threshold.shape, f32),
            pltpu.VMEM((core, core), bf16),
            pltpu.VMEM(kernels.shape, bf16),
            pltpu.VMEM(first_table.shape, bf16),
            pltpu.VMEM(later_table.shape, bf16),
            pltpu.VMEM((2, 3, MARGIN, 2 * band), bf16),
            pltpu.VMEM((2, 3, MARGIN, 2 * band), bf16),
            pltpu.VMEM((2, band, 2 * MARGIN), bf16),
            pltpu.VMEM((2, band, 2 * MARGIN), bf16),
            pltpu.VMEM((conds, grid, grid), f32),
            pltpu.VMEM((n_cond - 1, conds, grid, grid), f32),
            pltpu.SemaphoreType.DMA((8,)),
            pltpu.SemaphoreType.DMA((n_cond - 1, min(conds, 3))),
            pltpu.SemaphoreType.DMA,
            pltpu.VMEM((2 * MARGIN, 2 * band), bf16),
            pltpu.VMEM((2, band, 2 * band), f32),
            pltpu.VMEM(kernels.shape, f32),
            pltpu.VMEM(kernels.shape, f32),
        ],
        compiler_params=pltpu.CompilerParams(collective_id=0, has_side_effects=True),
    )(mask, kernels, socs_weight, dose, threshold, jnp.asarray(first_table), jnp.asarray(later_table))
    out = jax.ShapeDtypeStruct((1, share, core), f32)
    return pl.pallas_call(
        finish,
        out_shape=(out, out),
        in_specs=[vmem] * 2,
        out_specs=(anywhere, anywhere),
        scratch_shapes=[pltpu.VMEM((2, share, core), f32)],
    )(*(pltpu.with_memory_space_constraint(x, pltpu.VMEM) for x in (high, low)))


def solution(mesh):
    return jax.shard_map(
        on_device,
        mesh=mesh,
        in_specs=(
            P(("parts", "tile"), None, None),
            P("cond", None, None, None),
            P("cond", None),
            P("cond"),
            P("cond"),
        ),
        out_specs=(P(("parts", "tile"), "cond", None), P(("parts", "tile"), "cond", None)),
        check_vma=False,
    )
```
